512 devices in a mesh: gx: 16 (over y, x), gy: 16 (over z), gz: 2 (over core).
Axes of the slice: x: 4, y: 4, z: 16, core: 2. Of those that a mesh axis runs over, the one named last changes fastest.
Arguments:
- forcing: float32 [256, 1024, 256], P('gx', 'gy', 'gz'), may hold values from -6 to 6
- conductivity: float32 [32, 128, 32], P('gx', 'gy', 'gz'), may hold values from 0.5 to 4
- lower_bound: float32 [1], replicated, may hold values from 0.1 to 0.3
- upper_bound: float32 [1], replicated, may hold values from 1.6 to 2.4
Outputs:
- solution: float32 [256, 1024, 256], P('gx', 'gy', 'gz')
- ratios: float32 [2], replicated
The draws below stay inside these ranges and needn't reach their ends.
All inputs are finite; a program needn't handle non-finite values.
Results may differ from the reference program's by a relative error of at most 0.00012.
Values sent between devices are 32-bit elements; how exact they have to be, the bound alone decides.
A program may use at most 64 MiB of HBM per device.

```python
import math
import jax
import jax.numpy as jnp
import numpy as np
from jax import lax

NP = 8
SWEEPS = 2
EXG = 32
EYG = 128
EZG = 32


def block_levels(own_key, extent, split, least, high):
    def one(axis_at, parts):
        steps = jax.random.uniform(jax.random.fold_in(jax.random.fold_in(own_key, 6), axis_at), (parts,), jnp.float32, least / len(split), high / len(split))
        return jnp.repeat(jnp.exp(steps), extent[axis_at] // parts).reshape((-1,) + (1,) * (len(extent) - axis_at - 1))

    loudness = one(*split[0])
    for cut in split[1:]:
        loudness = loudness * one(*cut)
    return loudness


def bell_draw(rng, extent, deviation, bound, shards=(), dtype=jnp.bfloat16):
    values = deviation * jax.random.normal(rng, extent, jnp.float32)
    if shards:
        values = values * block_levels(rng, extent, shards, -0.22, 0.18)
    return jnp.clip(values, -bound, bound).astype(dtype)


def setup_inputs(seed: int = 0) -> dict:
    arg_keys = jax.random.split(jax.random.key(seed), 5)
    return {
        "forcing": bell_draw(arg_keys[0], (NP * EXG, NP * EYG, NP * EZG), 1.0, 6.0, ((0, 16), (1, 16), (2, 2)), jnp.float32),
        "conductivity": jnp.clip(jnp.exp(math.log(4.0) - 2.0794415 * jax.random.uniform(arg_keys[1], (EXG, EYG, EZG), jnp.float32) ** block_levels(arg_keys[1], (EXG, EYG, EZG), ((0, 16), (1, 16), (2, 2)), -0.2, 0.2)), 0.5, 4.0),
        "lower_bound": jnp.clip(jax.random.uniform(arg_keys[2], (1,), jnp.float32, 0.1, 0.3), 0.1, 0.3),
        "upper_bound": jnp.clip(jax.random.uniform(arg_keys[3], (1,), jnp.float32, 1.6, 2.4), 1.6, 2.4),
    }


gll_inner = [0.20929921790247888, 0.5917001814331423, 0.8717401485096066]

def gll_tables():
    degree_val = 7
    points = np.array([-1.0, -gll_inner[2], -gll_inner[1], -gll_inner[0], gll_inner[0], gll_inner[1], gll_inner[2], 1.0])
    previous = np.ones(8)
    values = points * 1.0
    for order in range(1, degree_val):
        following = ((2.0 * order + 1.0) * points * values - order * previous) / (order + 1.0)
        previous = values
        values = following
    weights = 2.0 / (degree_val * (degree_val + 1) * values ** 2)
    differ = points[:, None] - points[None, :]
    safe_gap = np.where(differ == 0.0, 1.0, differ)
    derivative = np.where(differ == 0.0, 0.0, values[:, None] / values[None, :] / safe_gap)
    corner_val = degree_val * (degree_val + 1) / 4.0
    ends_vec = np.concatenate([np.array([-corner_val]), np.zeros(6), np.array([corner_val])])
    index_row = np.arange(8)
    derivative = derivative + np.where(index_row[:, None] == index_row[None, :], ends_vec[None, :], 0.0)
    stiffness = derivative.T @ (weights[:, None] * derivative)
    return (weights, stiffness)

def edge_masks(length):
    positions = jnp.arange(length) % 8
    return ((positions == 0).astype(jnp.float32), (positions == 7).astype(jnp.float32))

def pair_sum(padded, which_axis, is_first, is_last):
    length = padded.shape[which_axis] - 2
    centre = lax.slice_in_dim(padded, 1, length + 1, axis=which_axis)
    upper_side = lax.slice_in_dim(padded, 2, length + 2, axis=which_axis)
    lower_side = lax.slice_in_dim(padded, 0, length, axis=which_axis)
    view_shape = [1] * padded.ndim
    view_shape[which_axis] = length
    return centre + jnp.reshape(is_last, view_shape) * upper_side + jnp.reshape(is_first, view_shape) * lower_side

def direct_sum(field):
    for which_axis in range(3):
        widths = [(0, 0), (0, 0), (0, 0)]
        widths[which_axis] = (1, 1)
        padded = jnp.pad(field, widths)
        is_first, is_last = edge_masks(field.shape[which_axis])
        field = pair_sum(padded, which_axis, is_first, is_last)
    return field

def inside(length):
    positions = jnp.arange(length)
    return ((positions > 0) & (positions < length - 1)).astype(jnp.float32)

def reference(forcing, conductivity, lower_bound, upper_bound):
    weights, stiffness = gll_tables()
    weights = jnp.asarray(weights, jnp.float32)
    stiffness = jnp.asarray(stiffness, jnp.float32)
    size_x, size_y, size_z = forcing.shape
    elem_x, elem_y, elem_z = conductivity.shape
    dirichlet = inside(size_x)[:, None, None] * inside(size_y)[None, :, None] * inside(size_z)[None, None, :]
    mults = []
    for length in (size_x, size_y, size_z):
        is_first, is_last = edge_masks(length)
        mults.append(1.0 + is_first + is_last)
    inv_mult = 1.0 / (mults[0][:, None, None] * mults[1][None, :, None] * mults[2][None, None, :])
    high = lax.Precision.HIGHEST
    wgt_i = weights[:, None, None, None, None]
    wgt_j = weights[None, None, :, None, None]
    wgt_k = weights[None, None, None, None, :]
    stiff_diag = jnp.diagonal(stiffness)
    diag_i = stiff_diag[:, None, None, None, None]
    diag_j = stiff_diag[None, None, :, None, None]
    diag_k = stiff_diag[None, None, None, None, :]

    def one_slab(pair):
        block, cond = pair
        blocks = block.reshape(8, elem_y, 8, elem_z, 8)
        along_x = jnp.einsum('pi,iejfk->pejfk', stiffness, blocks, precision=high)
        along_y = jnp.einsum('qj,iejfk->ieqfk', stiffness, blocks, precision=high)
        along_z = jnp.einsum('rk,iejfk->iejfr', stiffness, blocks, precision=high)
        summed = along_x * wgt_j * wgt_k + wgt_i * along_y * wgt_k + wgt_i * wgt_j * along_z
        return (cond[None, :, None, :, None] * summed).reshape(8, size_y, size_z)

    def local_apply(field):
        slabs = field.reshape(elem_x, 8, size_y, size_z)
        return lax.map(one_slab, (slabs, conductivity)).reshape(size_x, size_y, size_z)

    def diag_slab(cond):
        summed = diag_i * wgt_j * wgt_k + wgt_i * diag_j * wgt_k + wgt_i * wgt_j * diag_k
        return (cond[None, :, None, :, None] * summed).reshape(8, size_y, size_z)
    diag_local = lax.map(diag_slab, conductivity).reshape(size_x, size_y, size_z)
    source = dirichlet * direct_sum(forcing)
    inverse = dirichlet / direct_sum(diag_local)

    def operate(field):
        return dirichlet * direct_sum(local_apply(field))
    centre_val = (upper_bound[0] + lower_bound[0]) / 2.0
    half_width = (upper_bound[0] - lower_bound[0]) / 2.0
    rho_first = half_width / centre_val
    rho_second = 1.0 / (2.0 * centre_val / half_width - rho_first)
    source_sq = jnp.sum(source * source * inv_mult)
    solution = jnp.zeros_like(source)
    residual = source
    ratios = []
    for sweep in range(SWEEPS):
        update = inverse * residual / centre_val
        solution = solution + update
        residual = residual - operate(update)
        update = rho_second * rho_first * update + 2.0 * rho_second / half_width * inverse * residual
        solution = solution + update
        residual = residual - operate(update)
        ratios.append(jnp.sqrt(jnp.sum(residual * residual * inv_mult) / source_sq))
    return (solution, jnp.stack(ratios))
```

```python
import functools

import jax
import jax.numpy as jnp
import numpy as np
from jax import lax
from jax.experimental import pallas as pl
from jax.experimental.pallas import tpu as pltpu
from jax.sharding import PartitionSpec as P

MESH = pl.DeviceIdType.MESH
F32 = jnp.float32
BF16 = jnp.bfloat16
ROUNDS = 4

gll_inner = [0.20929921790247888, 0.5917001814331423, 0.8717401485096066]


def gll_tables():
    degree_val = 7
    points = np.array(
        [
            -1.0,
            -gll_inner[2],
            -gll_inner[1],
            -gll_inner[0],
            gll_inner[0],
            gll_inner[1],
            gll_inner[2],
            1.0,
        ]
    )
    previous = np.ones(8)
    values = points * 1.0
    for order in range(1, degree_val):
        following = ((2.0 * order + 1.0) * points * values - order * previous) / (order + 1.0)
        previous = values
        values = following
    weights = 2.0 / (degree_val * (degree_val + 1) * values**2)
    differ = points[:, None] - points[None, :]
    safe_gap = np.where(differ == 0.0, 1.0, differ)
    derivative = np.where(differ == 0.0, 0.0, values[:, None] / values[None, :] / safe_gap)
    corner_val = degree_val * (degree_val + 1) / 4.0
    ends_vec = np.concatenate([np.array([-corner_val]), np.zeros(6), np.array([corner_val])])
    index_row = np.arange(8)
    derivative = derivative + np.where(
        index_row[:, None] == index_row[None, :], ends_vec[None, :], 0.0
    )
    stiffness = derivative.T @ (weights[:, None] * derivative)
    return (weights, stiffness)


WEIGHTS, STIFF = gll_tables()
STIFF = 0.5 * (STIFF + STIFF[::-1, ::-1])
WEIGHTS = 0.5 * (WEIGHTS + WEIGHTS[::-1])


def halves(table):
    high = table.astype(np.float32).astype(jnp.dtype(BF16)).astype(np.float64)
    return high, table - high


def bf16_tables():
    scaled = STIFF / WEIGHTS[:, None]
    wide_z = np.kron(np.eye(16), scaled.T)
    high, low = halves(wide_z)
    along_z = np.block([[high, low], [high, np.zeros_like(low)]])
    wide_y = np.kron(np.eye(8), scaled)
    high, low = halves(wide_y)
    along_y = np.concatenate([high, high, low, np.zeros_like(low)], axis=1)
    return np.concatenate([along_z, along_y], axis=0).astype(np.float32)


def f32_tables():
    spread = np.kron(np.eye(16), np.ones((1, 8)))
    w, s = WEIGHTS, np.diagonal(STIFF)
    lanes = lambda v: np.tile(v, 16)[None, :]
    col = lambda v: v[:, None]
    parts = [spread, col(w) * lanes(w)]
    for p in range(8):
        diag = s[p] * col(w) * lanes(w) + w[p] * (col(s) * lanes(w) + col(w) * lanes(s))
        parts.append(1.0 / diag)
    return np.concatenate(parts, axis=0).astype(np.float32)


def smoother(
    nx,
    ny,
    f_ref,
    c_ref,
    lo_ref,
    up_ref,
    kb_ref,
    kf_ref,
    out_ref,
    ratio_ref,
    fb,
    xe0,
    yb0,
    y0,
    xy0,
    u,
    r,
    sol,
    inv,
    cb,
    wn,
    db,
    uz,
    yz,
    kb,
    kf,
    sx,
    rx,
    sy,
    ry,
    sd,
    rd,
    v1,
    a1,
    v2,
    a2,
    load_sem,
    send0,
    recv0,
    sends,
    recvs,
    out_send,
    out_recv,
    own_sem,
    s1_sem,
    r1_sem,
    s2_sem,
    r2_sem,
    far_y,
    far_x,
):
    gx = lax.axis_index("gx")
    gy = lax.axis_index("gy")
    t = lax.axis_index("gz")

    def at(dx, dy, core):
        return {"gx": lax.rem(gx + dx + nx, nx), "gy": lax.rem(gy + dy + ny, ny), "gz": core}

    def remote(src, dst, ss, rs, dev):
        return pltpu.make_async_remote_copy(
            src_ref=src, dst_ref=dst, send_sem=ss, recv_sem=rs, device_id=dev, device_id_type=MESH
        )

    barrier = pltpu.get_barrier_semaphore()
    count = 0
    for dx in (0, -1, 1):
        for dy in (0, -1, 1):
            for core in (1 - t, t):
                if dx == 0 and dy == 0 and core is t:
                    continue
                pl.semaphore_signal(
                    barrier, inc=1, device_id=at(dx, dy, core), device_id_type=MESH
                )
                count += 1

    loads = [
        pltpu.make_async_copy(f_ref, fb.at[t, :, pl.ds(0, 64)], load_sem.at[0]),
        pltpu.make_async_copy(kf_ref, kf, load_sem.at[1]),
        pltpu.make_async_copy(kb_ref, kb, load_sem.at[2]),
    ]
    for copy in loads:
        copy.start()

    row = lax.broadcasted_iota(jnp.int32, (8, 128), 0)
    lane = lax.broadcasted_iota(jnp.int32, (8, 128), 1)

    def z_sum(d0, d1):
        at_lane = lax.broadcasted_iota(jnp.int32, d0.shape, 1)
        k = lax.rem(at_lane, 8)
        ends = (k == 0) | (k == 7)
        up = k == 7
        axis = 1
        nxt0 = pltpu.roll(d0, 127, axis)
        nxt1 = pltpu.roll(d1, 127, axis)
        prv0 = pltpu.roll(d0, 1, axis)
        prv1 = pltpu.roll(d1, 1, axis)
        s0 = jnp.where(at_lane == 127, nxt1, jnp.where(up, nxt0, prv0))
        s1 = jnp.where(at_lane == 0, prv0, jnp.where(up, nxt1, prv1))
        zero = jnp.zeros_like(d0)
        return d0 + jnp.where(ends, s0, zero), d1 + jnp.where(ends, s1, zero)

    def spread_rows(value):
        return jnp.broadcast_to(value, (8, 128))

    loads[1].wait()
    ce = jnp.dot(
        c_ref[...].reshape(16, 16),
        kf[0:16, :],
        precision=lax.Precision.HIGHEST,
        preferred_element_type=F32,
    )
    for x, e in ((0, 0), (7, 0), (8, 1), (15, 1)):
        fb[t, x, 64:72, :] = ce[e * 8 : e * 8 + 8]
    loads[0].wait()
    for side, y in ((0, 0), (1, 63)):
        for b in range(2):
            for p in range(9):
                x = 15 - p if b else p
                yb0[side, b, p : p + 1, :] = fb[t, x, y : y + 1, :]
            e = 7 * side
            yb0[side, b, 9:10, :] = ce[b * 8 + e : b * 8 + e + 1]
            yb0[side, b, 10:11, :] = ce[(1 - b) * 8 + e : (1 - b) * 8 + e + 1]

    pl.semaphore_wait(barrier, count)

    mine = pl.ds(7 * (1 - t), 9)
    theirs = pl.ds(7 * t, 9)
    first = [
        remote(yb0.at[1, 1], xy0.at[0, t], send0.at[0], recv0.at[7 + t], at(1, 1, 0)),
        remote(yb0.at[0, 1], xy0.at[1, t], send0.at[1], recv0.at[9 + t], at(1, -1, 0)),
        remote(yb0.at[1, 0], xy0.at[0, t], send0.at[2], recv0.at[7 + t], at(-1, 1, 1)),
        remote(yb0.at[0, 0], xy0.at[1, t], send0.at[3], recv0.at[9 + t], at(-1, -1, 1)),
        remote(fb.at[t, 15], xe0.at[t], send0.at[4], recv0.at[1 + t], at(1, 0, 0)),
        remote(fb.at[t, 0], xe0.at[t], send0.at[5], recv0.at[1 + t], at(-1, 0, 1)),
        remote(fb.at[t, mine], fb.at[t, mine], send0.at[6], recv0.at[0], at(0, 0, 1 - t)),
        remote(yb0.at[1, 0], y0.at[0, t], send0.at[7], recv0.at[3 + t], at(0, 1, 0)),
        remote(yb0.at[1, 1], y0.at[0, t], send0.at[8], recv0.at[3 + t], at(0, 1, 1)),
        remote(yb0.at[0, 0], y0.at[1, t], send0.at[9], recv0.at[5 + t], at(0, -1, 0)),
        remote(yb0.at[0, 1], y0.at[1, t], send0.at[10], recv0.at[5 + t], at(0, -1, 1)),
    ]
    for copy in first:
        copy.start()

    def ring_signal(sem, axis, reach):
        for step in (reach, -reach):
            dev = at(step, 0, t) if axis == "gx" else at(0, step, t)
            pl.semaphore_signal(sem, inc=1, device_id=dev, device_id_type=MESH)

    hops_x = [h for h in (1, 2, 4, 8) if h < max(nx // 2, 1)]
    hops_y = [h for h in (1, 2, 4, 8) if h < max(ny // 2, 1)]

    def reach_step(i):
        if i > 0:
            if i - 1 < len(hops_x):
                pl.semaphore_wait(far_x.at[i - 1], 2)
            if i - 1 < len(hops_y):
                pl.semaphore_wait(far_y.at[i - 1], 2)
        if i < len(hops_x):
            ring_signal(far_x.at[i], "gx", hops_x[i])
        if i < len(hops_y):
            ring_signal(far_y.at[i], "gy", hops_y[i])

    reach_step(0)

    low = lo_ref[0]
    high = up_ref[0]
    centre = (high + low) / 2.0
    half = (high - low) / 2.0
    rho1 = half / centre
    rho2 = 1.0 / (2.0 * centre / half - rho1)
    first_scale = 1.0 / centre
    keep_scale = rho2 * rho1
    second_scale = 2.0 * rho2 / half

    last_y = ny * 64 - 1
    outer_x = jnp.where(t == 0, gx == 0, gx == nx - 1)
    inner_x = 1.0 - outer_x.astype(F32)
    z_half = jnp.where((lax.rem(lane, 8) == 0) | (lax.rem(lane, 8) == 7), 0.5, 1.0)
    yz_half = z_half * jnp.where((row == 0) | (row == 7), 0.5, 1.0)
    bound = {}
    for h in range(2):
        for e in range(8):
            keep = lane != (127 if h else 0)
            if e == 0:
                keep = keep & ((row + gy * 64) != 0)
            if e == 7:
                keep = keep & ((row + gy * 64 + 56) != last_y)
            bound[h, e] = jnp.where(keep, 1.0, 0.0)
            wn[h, e * 8 : e * 8 + 8, :] = bound[h, e] * yz_half

    def wait_for(dst, sem):
        remote(dst, dst, send0.at[0], sem, at(0, 0, 1 - t)).wait_recv()

    other = 1 - t
    wait_for(fb.at[other, theirs], recv0.at[0])
    for h in range(2):
        wait_for(xe0.at[h], recv0.at[1 + h])
        for side in range(2):
            wait_for(y0.at[side, h], recv0.at[3 + 2 * side + h])
            wait_for(xy0.at[side, h], recv0.at[7 + 2 * side + h])

    def plane(p):
        return p + t * (15 - 2 * p)

    def y_sum(rows_of):
        rows = [rows_of(0), rows_of(1)]
        for h in range(2):
            for p in range(8):
                a = db[h, p, pl.ds(7, 8, stride=8), :]
                b = db[h, p, pl.ds(0, 8, stride=8), :]
                from_high = spread_rows(rows[1][h][p : p + 1])
                from_low = spread_rows(rows[0][h][p : p + 1])
                up = jnp.where(row == 7, from_high, pltpu.roll(b, 7, 0))
                down = jnp.where(row == 0, from_low, pltpu.roll(a, 1, 0))
                db[h, p, pl.ds(7, 8, stride=8), :] = a + up
                db[h, p, pl.ds(0, 8, stride=8), :] = b + down

    for p in range(8):
        raw = []
        for h in range(2):
            d = fb[h, plane(p), 0:64, :]
            if p == 0:
                d = d + xe0[h, 0:64, :]
            if p == 7:
                d = d + fb[h, plane(8), 0:64, :]
            raw.append(d)
        db[0, p], db[1, p] = z_sum(*raw)

    def first_rows(side):
        raw = []
        for h in range(2):
            d = y0[side, h, 0:8, :]
            d = d + jnp.where(row == 0, spread_rows(xy0[side, h, 0:1, :]), 0.0)
            d = d + jnp.where(row == 7, spread_rows(y0[side, h, 8:9, :]), 0.0)
            raw.append(d)
        return z_sum(*raw)

    y_sum(first_rows)

    weight_jk = kf[16:24, :]
    for variant in range(3):
        own = [fb[h, plane(0), 64:72, :] for h in range(2)]
        near = [[spread_rows(y0[s, h, 9:10, :]) for h in range(2)] for s in range(2)]
        if variant == 0:
            for h in range(2):
                for e in range(8):
                    cb[h, e * 8 : e * 8 + 8, :] = spread_rows(own[h][e : e + 1]) * weight_jk
        if variant == 1:
            own = [own[h] + xe0[h, 64:72, :] for h in range(2)]
            near = [
                [near[s][h] + spread_rows(xy0[s, h, 9:10, :]) for h in range(2)] for s in range(2)
            ]
        if variant == 2:
            own = [own[h] + fb[h, plane(8), 64:72, :] for h in range(2)]
            near = [
                [near[s][h] + spread_rows(y0[s, h, 10:11, :]) for h in range(2)] for s in range(2)
            ]
        own = z_sum(*own)
        near = [z_sum(*pair) for pair in near]
        for h in range(2):
            a = own[h] + jnp.where(row == 7, near[1][h], pltpu.roll(own[h], 7, 0))
            b = own[h] + jnp.where(row == 0, near[0][h], pltpu.roll(own[h], 1, 0))
            for e in range(8):
                one = slice(e, e + 1)
                tile = jnp.where(
                    row == 7,
                    spread_rows(a[one]),
                    jnp.where(row == 0, spread_rows(b[one]), spread_rows(own[h][one])),
                )
                flip = bound[h, e] / tile
                if variant == 1:
                    flip = flip * inner_x
                for p in {0: range(1, 7), 1: (0,), 2: (7,)}[variant]:
                    inv[h, p, e * 8 : e * 8 + 8, :] = flip * kf[24 + 8 * p : 32 + 8 * p, :]

    reach_step(1)
    loads[2].wait()

    stiff = STIFF
    even = [[float(stiff[p, i] + stiff[p, 7 - i]) / 2 for i in range(4)] for p in range(4)]
    odd = [[float(stiff[p, i] - stiff[p, 7 - i]) / 2 for i in range(4)] for p in range(4)]

    def norm_of(acc):
        return jnp.sum(acc)

    def update(step):
        total = jnp.zeros((8, 128), F32)
        for h in range(2):
            for p in range(8):
                if step == 0:
                    res = db[h, p]
                else:
                    res = r[h, p] - db[h, p]
                if step % 2 == 0:
                    square = res * res * wn[h]
                    part = jnp.sum(square.reshape(8, 8, 128), axis=0)
                    if p == 0:
                        part = part * (0.5 * inner_x)
                    if p == 7:
                        part = part * 0.5
                    total = total + part
                if step == ROUNDS:
                    continue
                r[h, p] = res
                if step % 2 == 0:
                    new = inv[h, p] * (res * first_scale)
                else:
                    new = keep_scale * u[h, p] + second_scale * (inv[h, p] * res)
                u[h, p] = new
                home = p + t * (7 - 2 * p)
                sol[h, home] = new if step == 0 else sol[h, home] + new
                top = new.astype(BF16)
                uz[h, p, :, 0:128] = top
                uz[h, p, :, 128:256] = (new - top.astype(F32)).astype(BF16)
        return total

    def apply(k):
        along_z = kb[0:256, :]
        for h in range(2):
            out = jnp.dot(uz[h].reshape(512, 256), along_z, preferred_element_type=F32)
            yz[h] = (out[:, 0:128] + out[:, 128:256]).reshape(8, 64, 128)
        along_y = kb[256:320, 0:192]
        for p in range(8):
            top = jnp.concatenate([uz[0, p, :, 0:128], uz[1, p, :, 0:128]], axis=1)
            low_part = jnp.concatenate([uz[0, p, :, 128:256], uz[1, p, :, 128:256]], axis=1)
            both = jnp.concatenate([top, low_part, top], axis=0)
            out = jnp.dot(along_y, both, preferred_element_type=F32)
            for h in range(2):
                yz[h, p] = yz[h, p] + out[:, h * 128 : h * 128 + 128]
        for h in range(2):
            for e in range(8):
                rows = pl.ds(e * 8, 8)
                val = [u[h, p, rows, :] for p in range(8)]
                plus = [(val[i] + val[7 - i]) for i in range(4)]
                minus = [(val[i] - val[7 - i]) for i in range(4)]
                coef = cb[h, rows, :]
                for p in range(4):
                    ev = sum(even[p][i] * plus[i] for i in range(4))
                    od = sum(odd[p][i] * minus[i] for i in range(4))
                    w = float(WEIGHTS[p])
                    d_low = coef * (ev + od + w * yz[h, p, rows, :])
                    d_high = coef * (ev - od + w * yz[h, 7 - p, rows, :])
                    db[h, p, rows, :] = d_low
                    db[h, 7 - p, rows, :] = d_high
                    if p == 0:
                        sx[k, 0, h, rows, :] = d_low
                        sx[k, 1, h, rows, :] = d_high
                    if e in (0, 7):
                        side = 0 if e == 0 else 1
                        j = 0 if e == 0 else 7
                        sy[k, side, h, p : p + 1, :] = d_low[j : j + 1]
                        sy[k, side, h, 7 - p : 8 - p, :] = d_high[j : j + 1]
                        if p == 0:
                            sd[k, 0, side, h : h + 1, :] = d_low[j : j + 1]
                            sd[k, 1, side, h : h + 1, :] = d_high[j : j + 1]

    def messages(k):
        ss = sends.at[k]
        rs = recvs.at[k]
        ext = 2 * t - 1
        return [
            remote(sd.at[k, 0, 0], rd.at[k, 0, 1], ss.at[4], rs.at[5], at(ext, -1, other)),
            remote(sd.at[k, 0, 1], rd.at[k, 0, 0], ss.at[5], rs.at[4], at(ext, 1, other)),
            remote(sx.at[k, 0], rx.at[k, 0], ss.at[0], rs.at[0], at(ext, 0, other)),
            remote(sd.at[k, 1, 0], rd.at[k, 1, 1], ss.at[6], rs.at[7], at(0, -1, other)),
            remote(sd.at[k, 1, 1], rd.at[k, 1, 0], ss.at[7], rs.at[6], at(0, 1, other)),
            remote(sy.at[k, 0], ry.at[k, 1], ss.at[2], rs.at[3], at(0, -1, t)),
            remote(sy.at[k, 1], ry.at[k, 0], ss.at[3], rs.at[2], at(0, 1, t)),
            remote(sx.at[k, 1], rx.at[k, 1], ss.at[1], rs.at[1], at(0, 0, other)),
        ]

    def assemble(k):
        copies = messages(k)
        for copy in copies:
            copy.start()
        for p in range(1, 7):
            db[0, p], db[1, p] = z_sum(db[0, p], db[1, p])
        for copy in copies:
            copy.wait_recv()
        for side, p in ((0, 0), (1, 7)):
            db[0, p], db[1, p] = z_sum(
                db[0, p] + rx[k, side, 0], db[1, p] + rx[k, side, 1]
            )

        def rows_of(side):
            raw = []
            for h in range(2):
                d = ry[k, side, h]
                d = d + jnp.where(row == 0, spread_rows(rd[k, 0, side, h : h + 1, :]), 0.0)
                d = d + jnp.where(row == 7, spread_rows(rd[k, 1, side, h : h + 1, :]), 0.0)
                raw.append(d)
            return z_sum(*raw)

        y_sum(rows_of)
        return copies

    sent = list(first)
    norms = []
    tail = []
    for step in range(ROUNDS):
        total = update(step)
        if step % 2 == 0:
            norms.append(norm_of(total))
        if step == ROUNDS - 1:
            half_rows = pl.ds(8 * t, 8)
            away = remote(
                sol.at[other], out_ref.at[half_rows], out_send, out_recv, at(0, 0, other)
            )
            home = pltpu.make_async_copy(sol.at[t], out_ref.at[half_rows], own_sem)
            away.start()
            home.start()
            tail = [away, home]
        apply(step)
        sent += assemble(step)
        reach_step(step + 2)
    norms.append(norm_of(update(ROUNDS)))

    lane1 = lax.broadcasted_iota(jnp.int32, (1, 128), 1)
    line = jnp.where(lane1 == 0, norms[0], jnp.where(lane1 == 1, norms[1], norms[2]))
    v1[...] = line
    hops = []
    for o in range(1, ny):
        hops.append(remote(v1, a1.at[gy], s1_sem.at[o], r1_sem.at[gy], at(0, o, t)))
    for copy in hops:
        copy.start()
    a1[gy] = line
    for o in range(1, ny):
        source = lax.rem(gy + o, ny)
        wait_for(a1.at[source], r1_sem.at[source])
    line = jnp.sum(a1[...], axis=0)
    v2[...] = line
    slot = gx * 2 + t
    wide = []
    for o in range(0, nx):
        for flip in range(2):
            if o == 0 and flip == 0:
                continue
            core = other if flip else t
            i = 2 * o + flip
            wide.append(remote(v2, a2.at[slot], s2_sem.at[i], r2_sem.at[slot], at(o, 0, core)))
    for copy in wide:
        copy.start()
    a2[slot] = line
    for o in range(0, nx):
        for flip in range(2):
            if o == 0 and flip == 0:
                continue
            source = lax.rem(gx + o, nx) * 2 + (other if flip else t)
            wait_for(a2.at[source], r2_sem.at[source])
    line = jnp.sum(a2[...], axis=0)
    whole = line[0, 0]
    ratio_ref[...] = jnp.sqrt(line / whole)

    tail[0].wait_recv()
    tail[1].wait()
    for copy in sent + hops + wide + tail[:1]:
        copy.wait_send()


def per_device(nx, ny, forcing, conductivity, lower_bound, upper_bound):
    vmem = lambda *shape: pltpu.VMEM(shape, F32)
    dma = lambda *shape: pltpu.SemaphoreType.DMA(shape)
    scratch = [
        vmem(2, 16, 72, 128),
        vmem(2, 72, 128),
        vmem(2, 2, 16, 128),
        vmem(2, 2, 16, 128),
        vmem(2, 2, 16, 128),
        vmem(2, 8, 64, 128),
        vmem(2, 8, 64, 128),
        vmem(2, 8, 64, 128),
        vmem(2, 8, 64, 128),
        vmem(2, 64, 128),
        vmem(2, 64, 128),
        vmem(2, 8, 64, 128),
        pltpu.VMEM((2, 8, 64, 256), BF16),
        vmem(2, 8, 64, 128),
        pltpu.VMEM((320, 256), BF16),
        vmem(88, 128),
        vmem(ROUNDS, 2, 2, 64, 128),
        vmem(ROUNDS, 2, 2, 64, 128),
        vmem(ROUNDS, 2, 2, 8, 128),
        vmem(ROUNDS, 2, 2, 8, 128),
        vmem(ROUNDS, 2, 2, 2, 128),
        vmem(ROUNDS, 2, 2, 2, 128),
        vmem(1, 128),
        vmem(ny, 1, 128),
        vmem(1, 128),
        vmem(2 * nx, 1, 128),
        dma(3),
        dma(11),
        dma(11),
        dma(ROUNDS, 8),
        dma(ROUNDS, 8),
        dma(),
        dma(),
        dma(),
        dma(ny),
        dma(ny),
        dma(2 * nx),
        dma(2 * nx),
        pltpu.SemaphoreType.REGULAR((4,)),
        pltpu.SemaphoreType.REGULAR((4,)),
    ]
    anywhere = pl.BlockSpec(memory_space=pl.ANY)
    in_vmem = pl.BlockSpec(memory_space=pltpu.VMEM)
    in_smem = pl.BlockSpec(memory_space=pltpu.SMEM)
    result, line = pl.pallas_call(
        functools.partial(smoother, nx, ny),
        out_shape=(
            jax.ShapeDtypeStruct(forcing.shape, F32),
            jax.ShapeDtypeStruct((1, 128), F32),
        ),
        in_specs=[anywhere, in_vmem, in_smem, in_smem, anywhere, anywhere],
        out_specs=(anywhere, in_vmem),
        scratch_shapes=scratch,
        compiler_params=pltpu.CompilerParams(collective_id=0, has_side_effects=True),
    )(
        forcing,
        conductivity,
        lower_bound,
        upper_bound,
        jnp.asarray(bf16_tables(), BF16),
        jnp.asarray(f32_tables(), F32),
    )
    return result, line[0, 1:3]


def solution(mesh):
    spec = P("gx", "gy", "gz")
    return jax.shard_map(
        functools.partial(per_device, mesh.shape["gx"], mesh.shape["gy"]),
        mesh=mesh,
        in_specs=(spec, spec, P(), P()),
        out_specs=(spec, P()),
        check_vma=False,
    )
```

```python
import functools

import jax
import jax.numpy as jnp
import numpy as np
from jax import lax
from jax.experimental import pallas as pl
from jax.experimental.pallas import tpu as pltpu
from jax.sharding import PartitionSpec as P

MESH = pl.DeviceIdType.MESH
F32 = jnp.float32
BF16 = jnp.bfloat16
ROUNDS = 4

gll_inner = [0.20929921790247888, 0.5917001814331423, 0.8717401485096066]


def gll_tables():
    degree_val = 7
    points = np.array(
        [
            -1.0,
            -gll_inner[2],
            -gll_inner[1],
            -gll_inner[0],
            gll_inner[0],
            gll_inner[1],
            gll_inner[2],
            1.0,
        ]
    )
    previous = np.ones(8)
    values = points * 1.0
    for order in range(1, degree_val):
        following = ((2.0 * order + 1.0) * points * values - order * previous) / (order + 1.0)
        previous = values
        values = following
    weights = 2.0 / (degree_val * (degree_val + 1) * values**2)
    differ = points[:, None] - points[None, :]
    safe_gap = np.where(differ == 0.0, 1.0, differ)
    derivative = np.where(differ == 0.0, 0.0, values[:, None] / values[None, :] / safe_gap)
    corner_val = degree_val * (degree_val + 1) / 4.0
    ends_vec = np.concatenate([np.array([-corner_val]), np.zeros(6), np.array([corner_val])])
    index_row = np.arange(8)
    derivative = derivative + np.where(
        index_row[:, None] == index_row[None, :], ends_vec[None, :], 0.0
    )
    stiffness = derivative.T @ (weights[:, None] * derivative)
    return (weights, stiffness)


WEIGHTS, STIFF = gll_tables()
STIFF = 0.5 * (STIFF + STIFF[::-1, ::-1])
WEIGHTS = 0.5 * (WEIGHTS + WEIGHTS[::-1])


def halves(table):
    high = table.astype(np.float32).astype(jnp.dtype(BF16)).astype(np.float64)
    return high, table - high


def bf16_tables():
    scaled = STIFF / WEIGHTS[:, None]
    wide_z = np.kron(np.eye(16), scaled.T)
    high, low = halves(wide_z)
    along_z = np.block([[high, low], [high, np.zeros_like(low)]])
    wide_y = np.kron(np.eye(8), scaled)
    high, low = halves(wide_y)
    along_y = np.concatenate([high, high, low, np.zeros_like(low)], axis=1)
    return np.concatenate([along_z, along_y], axis=0).astype(np.float32)


def f32_tables():
    spread = np.kron(np.eye(16), np.ones((1, 8)))
    w, s = WEIGHTS, np.diagonal(STIFF)
    lanes = lambda v: np.tile(v, 16)[None, :]
    col = lambda v: v[:, None]
    parts = [spread, col(w) * lanes(w)]
    for p in range(8):
        diag = s[p] * col(w) * lanes(w) + w[p] * (col(s) * lanes(w) + col(w) * lanes(s))
        parts.append(1.0 / diag)
    return np.concatenate(parts, axis=0).astype(np.float32)


def smoother(
    nx,
    ny,
    f_ref,
    c_ref,
    lo_ref,
    up_ref,
    kb_ref,
    kf_ref,
    out_ref,
    ratio_ref,
    fb,
    xe0,
    yb0,
    y0,
    xy0,
    u,
    r,
    sol,
    inv,
    cb,
    wn,
    db,
    uz,
    yz,
    kb,
    kf,
    sx,
    rx,
    sy,
    ry,
    sd,
    rd,
    v1,
    a1,
    v2,
    a2,
    cv,
    lo_s,
    up_s,
    load_sem,
    send0,
    recv0,
    sends,
    recvs,
    out_send,
    out_recv,
    s1_sem,
    r1_sem,
    s2_sem,
    r2_sem,
    far_y,
    far_x,
):
    gx = lax.axis_index("gx")
    gy = lax.axis_index("gy")
    t = lax.axis_index("gz")

    def at(dx, dy, core):
        return {"gx": lax.rem(gx + dx + nx, nx), "gy": lax.rem(gy + dy + ny, ny), "gz": core}

    def remote(src, dst, ss, rs, dev):
        return pltpu.make_async_remote_copy(
            src_ref=src, dst_ref=dst, send_sem=ss, recv_sem=rs, device_id=dev, device_id_type=MESH
        )

    barrier = pltpu.get_barrier_semaphore()
    count = 0
    for dx in (-1, 1, 0):
        for dy in (-1, 1, 0):
            for core in (1 - t, t):
                if dx == 0 and dy == 0 and core is t:
                    continue
                pl.semaphore_signal(
                    barrier, inc=1, device_id=at(dx, dy, core), device_id_type=MESH
                )
                count += 1

    loads = [
        pltpu.make_async_copy(f_ref, fb.at[t, :, pl.ds(0, 64)], load_sem.at[0]),
        pltpu.make_async_copy(kf_ref, kf, load_sem.at[1]),
        pltpu.make_async_copy(kb_ref, kb, load_sem.at[2]),
        pltpu.make_async_copy(c_ref, cv, load_sem.at[3]),
        pltpu.make_async_copy(lo_ref, lo_s, load_sem.at[4]),
        pltpu.make_async_copy(up_ref, up_s, load_sem.at[5]),
    ]
    for copy in loads:
        copy.start()

    row = lax.broadcasted_iota(jnp.int32, (8, 128), 0)
    lane = lax.broadcasted_iota(jnp.int32, (8, 128), 1)

    def z_sum(d0, d1):
        at_lane = lax.broadcasted_iota(jnp.int32, d0.shape, 1)
        k = lax.rem(at_lane, 8)
        ends = (k == 0) | (k == 7)
        up = k == 7
        axis = 1
        nxt0 = pltpu.roll(d0, 127, axis)
        nxt1 = pltpu.roll(d1, 127, axis)
        prv0 = pltpu.roll(d0, 1, axis)
        prv1 = pltpu.roll(d1, 1, axis)
        s0 = jnp.where(at_lane == 127, nxt1, jnp.where(up, nxt0, prv0))
        s1 = jnp.where(at_lane == 0, prv0, jnp.where(up, nxt1, prv1))
        zero = jnp.zeros_like(d0)
        return d0 + jnp.where(ends, s0, zero), d1 + jnp.where(ends, s1, zero)

    def spread_rows(value):
        return jnp.broadcast_to(value, (8, 128))

    loads[1].wait()
    loads[3].wait()
    ce = jnp.dot(
        cv[...].reshape(16, 16),
        kf[0:16, :],
        precision=lax.Precision.HIGHEST,
        preferred_element_type=F32,
    )
    for x, e in ((0, 0), (7, 0), (8, 1), (15, 1)):
        fb[t, x, 64:72, :] = ce[e * 8 : e * 8 + 8]
    loads[0].wait()
    for side, y in ((0, 0), (1, 63)):
        for b in range(2):
            for p in range(9):
                x = 15 - p if b else p
                yb0[side, b, p : p + 1, :] = fb[t, x, y : y + 1, :]
            e = 7 * side
            yb0[side, b, 9:10, :] = ce[b * 8 + e : b * 8 + e + 1]
            yb0[side, b, 10:11, :] = ce[(1 - b) * 8 + e : (1 - b) * 8 + e + 1]

    pl.semaphore_wait(barrier, count)

    mine = pl.ds(7 * (1 - t), 9)
    theirs = pl.ds(7 * t, 9)
    first = [
        remote(yb0.at[1, 1], xy0.at[0, t], send0.at[0], recv0.at[7 + t], at(1, 1, 0)),
        remote(yb0.at[0, 1], xy0.at[1, t], send0.at[1], recv0.at[9 + t], at(1, -1, 0)),
        remote(yb0.at[1, 0], xy0.at[0, t], send0.at[2], recv0.at[7 + t], at(-1, 1, 1)),
        remote(yb0.at[0, 0], xy0.at[1, t], send0.at[3], recv0.at[9 + t], at(-1, -1, 1)),
        remote(fb.at[t, 15], xe0.at[t], send0.at[4], recv0.at[1 + t], at(1, 0, 0)),
        remote(fb.at[t, 0], xe0.at[t], send0.at[5], recv0.at[1 + t], at(-1, 0, 1)),
        remote(fb.at[t, mine], fb.at[t, mine], send0.at[6], recv0.at[0], at(0, 0, 1 - t)),
        remote(yb0.at[1, 0], y0.at[0, t], send0.at[7], recv0.at[3 + t], at(0, 1, 0)),
        remote(yb0.at[1, 1], y0.at[0, t], send0.at[8], recv0.at[3 + t], at(0, 1, 1)),
        remote(yb0.at[0, 0], y0.at[1, t], send0.at[9], recv0.at[5 + t], at(0, -1, 0)),
        remote(yb0.at[0, 1], y0.at[1, t], send0.at[10], recv0.at[5 + t], at(0, -1, 1)),
    ]
    for copy in first:
        copy.start()

    def ring_signal(sem, axis, reach):
        for step in (reach, -reach):
            dev = at(step, 0, t) if axis == "gx" else at(0, step, t)
            pl.semaphore_signal(sem, inc=1, device_id=dev, device_id_type=MESH)

    hops_x = [h for h in (1, 2, 4, 8) if h < max(nx // 2, 1)]
    hops_y = [h for h in (1, 2, 4, 8) if h < max(ny // 2, 1)]

    def reach_step(i):
        if i > 0:
            if i - 1 < len(hops_x):
                pl.semaphore_wait(far_x.at[i - 1], 2)
            if i - 1 < len(hops_y):
                pl.semaphore_wait(far_y.at[i - 1], 2)
        if i < len(hops_x):
            ring_signal(far_x.at[i], "gx", hops_x[i])
        if i < len(hops_y):
            ring_signal(far_y.at[i], "gy", hops_y[i])

    reach_step(0)

    loads[4].wait()
    loads[5].wait()
    low = lo_s[0]
    high = up_s[0]
    centre = (high + low) / 2.0
    half = (high - low) / 2.0
    rho1 = half / centre
    rho2 = 1.0 / (2.0 * centre / half - rho1)
    first_scale = 1.0 / centre
    keep_scale = rho2 * rho1
    second_scale = 2.0 * rho2 / half

    last_y = ny * 64 - 1
    outer_x = jnp.where(t == 0, gx == 0, gx == nx - 1)
    inner_x = 1.0 - outer_x.astype(F32)
    z_half = jnp.where((lax.rem(lane, 8) == 0) | (lax.rem(lane, 8) == 7), 0.5, 1.0)
    yz_half = z_half * jnp.where((row == 0) | (row == 7), 0.5, 1.0)
    bound = {}
    for h in range(2):
        for e in range(8):
            keep = lane != (127 if h else 0)
            if e == 0:
                keep = keep & ((row + gy * 64) != 0)
            if e == 7:
                keep = keep & ((row + gy * 64 + 56) != last_y)
            bound[h, e] = jnp.where(keep, 1.0, 0.0)
            wn[h, e * 8 : e * 8 + 8, :] = bound[h, e] * yz_half

    def wait_for(dst, sem):
        remote(dst, dst, send0.at[0], sem, at(0, 0, 1 - t)).wait_recv()

    def plane(p):
        return p + t * (15 - 2 * p)

    def y_own(planes):
        for h in range(2):
            for p in planes:
                a = db[h, p, pl.ds(7, 8, stride=8), :]
                b = db[h, p, pl.ds(0, 8, stride=8), :]
                db[h, p, pl.ds(7, 8, stride=8), :] = a + jnp.where(
                    row == 7, 0.0, pltpu.roll(b, 7, 0)
                )
                db[h, p, pl.ds(0, 8, stride=8), :] = b + jnp.where(
                    row == 0, 0.0, pltpu.roll(a, 1, 0)
                )

    def y_add(rows_of):
        low_rows, high_rows = rows_of(0), rows_of(1)
        for h in range(2):
            for p in range(8):
                one = slice(p, p + 1)
                db[h, p, 0:1, :] = db[h, p, 0:1, :] + low_rows[h][one]
                db[h, p, 63:64, :] = db[h, p, 63:64, :] + high_rows[h][one]

    other = 1 - t
    weight_jk = kf[16:24, :]
    wait_for(fb.at[other, theirs], recv0.at[0])
    own_c = [fb[h, plane(0), 64:72, :] for h in range(2)]
    int_c = [fb[h, plane(8), 64:72, :] for h in range(2)]
    for h in range(2):
        for e in range(8):
            cb[h, e * 8 : e * 8 + 8, :] = spread_rows(own_c[h][e : e + 1]) * weight_jk
    for p in range(1, 7):
        db[0, p], db[1, p] = z_sum(fb[0, plane(p), 0:64, :], fb[1, plane(p), 0:64, :])
    y_own(range(1, 7))
    db[0, 7], db[1, 7] = z_sum(
        *[fb[h, plane(7), 0:64, :] + fb[h, plane(8), 0:64, :] for h in range(2)]
    )
    for h in range(2):
        wait_for(xe0.at[h], recv0.at[1 + h])
        for side in range(2):
            wait_for(y0.at[side, h], recv0.at[3 + 2 * side + h])
            wait_for(xy0.at[side, h], recv0.at[7 + 2 * side + h])
    db[0, 0], db[1, 0] = z_sum(
        *[fb[h, plane(0), 0:64, :] + xe0[h, 0:64, :] for h in range(2)]
    )

    def first_rows(side):
        raw = []
        for h in range(2):
            d = y0[side, h, 0:8, :]
            d = d + jnp.where(row == 0, spread_rows(xy0[side, h, 0:1, :]), 0.0)
            d = d + jnp.where(row == 7, spread_rows(y0[side, h, 8:9, :]), 0.0)
            raw.append(d)
        return z_sum(*raw)

    y_own((0, 7))
    y_add(first_rows)

    for variant in range(3):
        own = own_c
        near = [[spread_rows(y0[s, h, 9:10, :]) for h in range(2)] for s in range(2)]
        if variant == 1:
            own = [own[h] + xe0[h, 64:72, :] for h in range(2)]
            near = [
                [near[s][h] + spread_rows(xy0[s, h, 9:10, :]) for h in range(2)] for s in range(2)
            ]
        if variant == 2:
            own = [own[h] + int_c[h] for h in range(2)]
            near = [
                [near[s][h] + spread_rows(y0[s, h, 10:11, :]) for h in range(2)] for s in range(2)
            ]
        own = z_sum(*own)
        near = [z_sum(*pair) for pair in near]
        for h in range(2):
            a = own[h] + jnp.where(row == 7, near[1][h], pltpu.roll(own[h], 7, 0))
            b = own[h] + jnp.where(row == 0, near[0][h], pltpu.roll(own[h], 1, 0))
            for e in range(8):
                one = slice(e, e + 1)
                tile = jnp.where(
                    row == 7,
                    spread_rows(a[one]),
                    jnp.where(row == 0, spread_rows(b[one]), spread_rows(own[h][one])),
                )
                flip = bound[h, e] / tile
                if variant == 1:
                    flip = flip * inner_x
                for p in {0: range(1, 7), 1: (0,), 2: (7,)}[variant]:
                    inv[h, p, e * 8 : e * 8 + 8, :] = flip * kf[24 + 8 * p : 32 + 8 * p, :]

    reach_step(1)
    loads[2].wait()

    stiff = STIFF
    even = [[float(stiff[p, i] + stiff[p, 7 - i]) / 2 for i in range(4)] for p in range(4)]
    odd = [[float(stiff[p, i] - stiff[p, 7 - i]) / 2 for i in range(4)] for p in range(4)]

    def norm_of(acc):
        return jnp.sum(acc)

    def update(step):
        total = jnp.zeros((8, 128), F32)
        for h in range(2):
            for p in range(8):
                if step == 0:
                    res = db[h, p]
                else:
                    res = r[h, p] - db[h, p]
                if step % 2 == 0:
                    square = res * res * wn[h]
                    part = jnp.sum(square.reshape(8, 8, 128), axis=0)
                    if p == 0:
                        part = part * (0.5 * inner_x)
                    if p == 7:
                        part = part * 0.5
                    total = total + part
                if step == ROUNDS:
                    continue
                r[h, p] = res
                if step % 2 == 0:
                    new = inv[h, p] * (res * first_scale)
                else:
                    new = keep_scale * u[h, p] + second_scale * (inv[h, p] * res)
                u[h, p] = new
                home = p + t * (7 - 2 * p)
                sol[h, home] = new if step == 0 else sol[h, home] + new
                top = new.astype(BF16)
                uz[h, p, :, 0:128] = top
                uz[h, p, :, 128:256] = (new - top.astype(F32)).astype(BF16)
        return total

    def apply(k):
        along_z = kb[0:256, :]
        for h in range(2):
            out = jnp.dot(uz[h].reshape(512, 256), along_z, preferred_element_type=F32)
            yz[h] = (out[:, 0:128] + out[:, 128:256]).reshape(8, 64, 128)
        along_y = kb[256:320, 0:192]
        for p in range(8):
            top = jnp.concatenate([uz[0, p, :, 0:128], uz[1, p, :, 0:128]], axis=1)
            low_part = jnp.concatenate([uz[0, p, :, 128:256], uz[1, p, :, 128:256]], axis=1)
            both = jnp.concatenate([top, low_part, top], axis=0)
            out = jnp.dot(along_y, both, preferred_element_type=F32)
            for h in range(2):
                yz[h, p] = yz[h, p] + out[:, h * 128 : h * 128 + 128]
        for h in range(2):
            for e in range(8):
                rows = pl.ds(e * 8, 8)
                val = [u[h, p, rows, :] for p in range(8)]
                plus = [(val[i] + val[7 - i]) for i in range(4)]
                minus = [(val[i] - val[7 - i]) for i in range(4)]
                coef = cb[h, rows, :]
                for p in range(4):
                    ev = sum(even[p][i] * plus[i] for i in range(4))
                    od = sum(odd[p][i] * minus[i] for i in range(4))
                    w = float(WEIGHTS[p])
                    d_low = coef * (ev + od + w * yz[h, p, rows, :])
                    d_high = coef * (ev - od + w * yz[h, 7 - p, rows, :])
                    db[h, p, rows, :] = d_low
                    db[h, 7 - p, rows, :] = d_high
                    if p == 0:
                        sx[k, 0, h, rows, :] = d_low
                        sx[k, 1, h, rows, :] = d_high
                    if e in (0, 7):
                        side = 0 if e == 0 else 1
                        j = 0 if e == 0 else 7
                        sy[k, side, h, p : p + 1, :] = d_low[j : j + 1]
                        sy[k, side, h, 7 - p : 8 - p, :] = d_high[j : j + 1]
                        if p == 0:
                            sd[k, 0, side, h : h + 1, :] = d_low[j : j + 1]
                            sd[k, 1, side, h : h + 1, :] = d_high[j : j + 1]

    def messages(k):
        ss = sends.at[k]
        rs = recvs.at[k]
        ext = 2 * t - 1
        return [
            remote(sd.at[k, 0, 0], rd.at[k, 0, 1], ss.at[4], rs.at[5], at(ext, -1, other)),
            remote(sd.at[k, 0, 1], rd.at[k, 0, 0], ss.at[5], rs.at[4], at(ext, 1, other)),
            remote(sx.at[k, 0], rx.at[k, 0], ss.at[0], rs.at[0], at(ext, 0, other)),
            remote(sd.at[k, 1, 0], rd.at[k, 1, 1], ss.at[6], rs.at[7], at(0, -1, other)),
            remote(sd.at[k, 1, 1], rd.at[k, 1, 0], ss.at[7], rs.at[6], at(0, 1, other)),
            remote(sy.at[k, 0], ry.at[k, 1], ss.at[2], rs.at[3], at(0, -1, t)),
            remote(sy.at[k, 1], ry.at[k, 0], ss.at[3], rs.at[2], at(0, 1, t)),
            remote(sx.at[k, 1], rx.at[k, 1], ss.at[1], rs.at[1], at(0, 0, other)),
        ]

    def assemble(k):
        copies = messages(k)
        for copy in copies:
            copy.start()
        for p in range(1, 7):
            db[0, p], db[1, p] = z_sum(db[0, p], db[1, p])
        y_own(range(1, 7))
        if k == ROUNDS - 1:
            for p in range(8):
                out_ref[8 * t + p] = sol[t, p]
        for copy in copies:
            copy.wait_recv()
        for side, p in ((0, 0), (1, 7)):
            db[0, p], db[1, p] = z_sum(
                db[0, p] + rx[k, side, 0], db[1, p] + rx[k, side, 1]
            )

        def rows_of(side):
            raw = []
            for h in range(2):
                d = ry[k, side, h]
                d = d + jnp.where(row == 0, spread_rows(rd[k, 0, side, h : h + 1, :]), 0.0)
                d = d + jnp.where(row == 7, spread_rows(rd[k, 1, side, h : h + 1, :]), 0.0)
                raw.append(d)
            return z_sum(*raw)

        y_own((0, 7))
        y_add(rows_of)
        return copies

    sent = list(first)
    norms = []
    tail = []
    for step in range(ROUNDS):
        total = update(step)
        if step % 2 == 0:
            norms.append(norm_of(total))
        if step == ROUNDS - 1:
            half_rows = pl.ds(8 * t, 8)
            away = remote(
                sol.at[other], out_ref.at[half_rows], out_send, out_recv, at(0, 0, other)
            )
            away.start()
            tail = [away]
        apply(step)
        sent += assemble(step)
        reach_step(step + 2)
    norms.append(norm_of(update(ROUNDS)))

    lane1 = lax.broadcasted_iota(jnp.int32, (1, 128), 1)
    line = jnp.where(lane1 == 0, norms[0], jnp.where(lane1 == 1, norms[1], norms[2]))
    v1[...] = line
    hops = []
    for o in range(1, ny):
        hops.append(remote(v1, a1.at[gy], s1_sem.at[o], r1_sem.at[gy], at(0, o, t)))
    for copy in hops:
        copy.start()
    a1[gy] = line
    for o in range(1, ny):
        source = lax.rem(gy + o, ny)
        wait_for(a1.at[source], r1_sem.at[source])
    line = jnp.sum(a1[...], axis=0)
    v2[...] = line
    slot = gx * 2 + t
    wide = []
    for o in range(0, nx):
        for flip in range(2):
            if o == 0 and flip == 0:
                continue
            core = other if flip else t
            i = 2 * o + flip
            wide.append(remote(v2, a2.at[slot], s2_sem.at[i], r2_sem.at[slot], at(o, 0, core)))
    for copy in wide:
        copy.start()
    a2[slot] = line
    for o in range(0, nx):
        for flip in range(2):
            if o == 0 and flip == 0:
                continue
            source = lax.rem(gx + o, nx) * 2 + (other if flip else t)
            wait_for(a2.at[source], r2_sem.at[source])
    line = jnp.sum(a2[...], axis=0)
    whole = line[0, 0]
    ratio_ref[...] = pltpu.roll(jnp.sqrt(line / whole), 127, 1)[:, 0:2]

    tail[0].wait_recv()
    for copy in sent + hops + wide + tail[:1]:
        copy.wait_send()


def per_device(nx, ny, forcing, conductivity, lower_bound, upper_bound):
    vmem = lambda *shape: pltpu.VMEM(shape, F32)
    dma = lambda *shape: pltpu.SemaphoreType.DMA(shape)
    scratch = [
        vmem(2, 16, 72, 128),
        vmem(2, 72, 128),
        vmem(2, 2, 16, 128),
        vmem(2, 2, 16, 128),
        vmem(2, 2, 16, 128),
        vmem(2, 8, 64, 128),
        vmem(2, 8, 64, 128),
        vmem(2, 8, 64, 128),
        vmem(2, 8, 64, 128),
        vmem(2, 64, 128),
        vmem(2, 64, 128),
        vmem(2, 8, 64, 128),
        pltpu.VMEM((2, 8, 64, 256), BF16),
        vmem(2, 8, 64, 128),
        pltpu.VMEM((320, 256), BF16),
        vmem(88, 128),
        vmem(ROUNDS, 2, 2, 64, 128),
        vmem(ROUNDS, 2, 2, 64, 128),
        vmem(ROUNDS, 2, 2, 8, 128),
        vmem(ROUNDS, 2, 2, 8, 128),
        vmem(ROUNDS, 2, 2, 2, 128),
        vmem(ROUNDS, 2, 2, 2, 128),
        vmem(1, 128),
        vmem(ny, 1, 128),
        vmem(1, 128),
        vmem(2 * nx, 1, 128),
        vmem(2, 8, 16),
        pltpu.SMEM((1,), F32),
        pltpu.SMEM((1,), F32),
        dma(6),
        dma(11),
        dma(11),
        dma(ROUNDS, 8),
        dma(ROUNDS, 8),
        dma(),
        dma(),
        dma(ny),
        dma(ny),
        dma(2 * nx),
        dma(2 * nx),
        pltpu.SemaphoreType.REGULAR((4,)),
        pltpu.SemaphoreType.REGULAR((4,)),
    ]
    anywhere = pl.BlockSpec(memory_space=pl.ANY)
    in_vmem = pl.BlockSpec(memory_space=pltpu.VMEM)
    result, line = pl.pallas_call(
        functools.partial(smoother, nx, ny),
        out_shape=(
            pltpu.VMEM(forcing.shape, F32),
            jax.ShapeDtypeStruct((1, 2), F32),
        ),
        in_specs=[anywhere] * 6,
        out_specs=(in_vmem, in_vmem),
        scratch_shapes=scratch,
        compiler_params=pltpu.CompilerParams(collective_id=0, has_side_effects=True),
    )(
        forcing,
        conductivity,
        lower_bound,
        upper_bound,
        jnp.asarray(bf16_tables(), BF16),
        jnp.asarray(f32_tables(), F32),
    )
    return result, line.reshape(2)


def solution(mesh):
    spec = P("gx", "gy", "gz")
    return jax.shard_map(
        functools.partial(per_device, mesh.shape["gx"], mesh.shape["gy"]),
        mesh=mesh,
        in_specs=(spec, spec, P(), P()),
        out_specs=(spec, P()),
        check_vma=False,
    )
```

```python
import functools

import jax
import jax.numpy as jnp
import numpy as np
from jax import lax
from jax.experimental import pallas as pl
from jax.experimental.pallas import tpu as pltpu
from jax.sharding import PartitionSpec as P

MESH = pl.DeviceIdType.MESH
F32 = jnp.float32
BF16 = jnp.bfloat16
ROUNDS = 4

gll_inner = [0.20929921790247888, 0.5917001814331423, 0.8717401485096066]


def gll_tables():
    degree_val = 7
    points = np.array(
        [
            -1.0,
            -gll_inner[2],
            -gll_inner[1],
            -gll_inner[0],
            gll_inner[0],
            gll_inner[1],
            gll_inner[2],
            1.0,
        ]
    )
    previous = np.ones(8)
    values = points * 1.0
    for order in range(1, degree_val):
        following = ((2.0 * order + 1.0) * points * values - order * previous) / (order + 1.0)
        previous = values
        values = following
    weights = 2.0 / (degree_val * (degree_val + 1) * values**2)
    differ = points[:, None] - points[None, :]
    safe_gap = np.where(differ == 0.0, 1.0, differ)
    derivative = np.where(differ == 0.0, 0.0, values[:, None] / values[None, :] / safe_gap)
    corner_val = degree_val * (degree_val + 1) / 4.0
    ends_vec = np.concatenate([np.array([-corner_val]), np.zeros(6), np.array([corner_val])])
    index_row = np.arange(8)
    derivative = derivative + np.where(
        index_row[:, None] == index_row[None, :], ends_vec[None, :], 0.0
    )
    stiffness = derivative.T @ (weights[:, None] * derivative)
    return (weights, stiffness)


WEIGHTS, STIFF = gll_tables()
STIFF = 0.5 * (STIFF + STIFF[::-1, ::-1])
WEIGHTS = 0.5 * (WEIGHTS + WEIGHTS[::-1])


def halves(table):
    high = table.astype(np.float32).astype(jnp.dtype(BF16)).astype(np.float64)
    return high, table - high


def bf16_tables():
    scaled = STIFF / WEIGHTS[:, None]
    wide_z = np.kron(np.eye(16), scaled.T)
    high, low = halves(wide_z)
    along_z = np.block([[high, low], [high, np.zeros_like(low)]])
    wide_y = np.kron(np.eye(8), scaled)
    high, low = halves(wide_y)
    along_y = np.concatenate([high, high, low, np.zeros_like(low)], axis=1)
    few_high, few_low = high[:32, :32], low[:32, :32]
    few = np.concatenate([few_high, few_high, few_low, np.zeros((32, 160))], axis=1)
    return np.concatenate([along_z, along_y, few], axis=0).astype(np.float32)


def f32_tables():
    spread = np.kron(np.eye(16), np.ones((1, 8)))
    w, s = WEIGHTS, np.diagonal(STIFF)
    lanes = lambda v: np.tile(v, 16)[None, :]
    col = lambda v: v[:, None]
    parts = [spread, col(w) * lanes(w)]
    for p in range(8):
        diag = s[p] * col(w) * lanes(w) + w[p] * (col(s) * lanes(w) + col(w) * lanes(s))
        parts.append(1.0 / diag)
    return np.concatenate(parts, axis=0).astype(np.float32)


def smoother(
    nx,
    ny,
    f_ref,
    c_ref,
    lo_ref,
    up_ref,
    kb_ref,
    kf_ref,
    out_ref,
    ratio_ref,
    fb,
    xe0,
    yb0,
    y0,
    xy0,
    u,
    r,
    sol,
    inv,
    cb,
    wn,
    db,
    uz,
    yz,
    kb,
    kf,
    sx,
    rx,
    sy,
    ry,
    sd,
    rd,
    v1,
    a1,
    v2,
    a2,
    cv,
    lo_s,
    up_s,
    load_sem,
    send0,
    recv0,
    sends,
    recvs,
    out_send,
    out_recv,
    s1_sem,
    r1_sem,
    s2_sem,
    r2_sem,
    far_y,
    far_x,
):
    gx = lax.axis_index("gx")
    gy = lax.axis_index("gy")
    t = lax.axis_index("gz")

    def at(dx, dy, core):
        return {"gx": lax.rem(gx + dx + nx, nx), "gy": lax.rem(gy + dy + ny, ny), "gz": core}

    def remote(src, dst, ss, rs, dev):
        return pltpu.make_async_remote_copy(
            src_ref=src, dst_ref=dst, send_sem=ss, recv_sem=rs, device_id=dev, device_id_type=MESH
        )

    barrier = pltpu.get_barrier_semaphore()
    count = 0
    for dx in (-1, 1, 0):
        for dy in (-1, 1, 0):
            for core in (1 - t, t):
                if dx == 0 and dy == 0 and core is t:
                    continue
                pl.semaphore_signal(
                    barrier, inc=1, device_id=at(dx, dy, core), device_id_type=MESH
                )
                count += 1

    loads = [
        pltpu.make_async_copy(f_ref, fb.at[t, :, pl.ds(0, 64)], load_sem.at[0]),
        pltpu.make_async_copy(kf_ref, kf, load_sem.at[1]),
        pltpu.make_async_copy(kb_ref, kb, load_sem.at[2]),
        pltpu.make_async_copy(c_ref, cv, load_sem.at[3]),
        pltpu.make_async_copy(lo_ref, lo_s, load_sem.at[4]),
        pltpu.make_async_copy(up_ref, up_s, load_sem.at[5]),
    ]
    for copy in loads:
        copy.start()

    row = lax.broadcasted_iota(jnp.int32, (8, 128), 0)
    lane = lax.broadcasted_iota(jnp.int32, (8, 128), 1)

    def z_sum(d0, d1):
        at_lane = lax.broadcasted_iota(jnp.int32, d0.shape, 1)
        k = lax.rem(at_lane, 8)
        ends = (k == 0) | (k == 7)
        up = k == 7
        axis = 1
        nxt0 = pltpu.roll(d0, 127, axis)
        nxt1 = pltpu.roll(d1, 127, axis)
        prv0 = pltpu.roll(d0, 1, axis)
        prv1 = pltpu.roll(d1, 1, axis)
        s0 = jnp.where(at_lane == 127, nxt1, jnp.where(up, nxt0, prv0))
        s1 = jnp.where(at_lane == 0, prv0, jnp.where(up, nxt1, prv1))
        zero = jnp.zeros_like(d0)
        return d0 + jnp.where(ends, s0, zero), d1 + jnp.where(ends, s1, zero)

    def spread_rows(value):
        return jnp.broadcast_to(value, (8, 128))

    loads[1].wait()
    loads[3].wait()
    ce = jnp.dot(
        cv[...].reshape(16, 16),
        kf[0:16, :],
        precision=lax.Precision.HIGHEST,
        preferred_element_type=F32,
    )
    for x, e in ((0, 0), (7, 0), (8, 1), (15, 1)):
        fb[t, x, 64:72, :] = ce[e * 8 : e * 8 + 8]
    loads[0].wait()
    for side, y in ((0, 0), (1, 63)):
        for b in range(2):
            for p in range(9):
                x = 15 - p if b else p
                yb0[side, b, p : p + 1, :] = fb[t, x, y : y + 1, :]
            e = 7 * side
            yb0[side, b, 9:10, :] = ce[b * 8 + e : b * 8 + e + 1]
            yb0[side, b, 10:11, :] = ce[(1 - b) * 8 + e : (1 - b) * 8 + e + 1]

    pl.semaphore_wait(barrier, count)

    mine = pl.ds(7 * (1 - t), 9)
    theirs = pl.ds(7 * t, 9)
    first = [
        remote(yb0.at[1, 1], xy0.at[0, t], send0.at[0], recv0.at[7 + t], at(1, 1, 0)),
        remote(yb0.at[0, 1], xy0.at[1, t], send0.at[1], recv0.at[9 + t], at(1, -1, 0)),
        remote(yb0.at[1, 0], xy0.at[0, t], send0.at[2], recv0.at[7 + t], at(-1, 1, 1)),
        remote(yb0.at[0, 0], xy0.at[1, t], send0.at[3], recv0.at[9 + t], at(-1, -1, 1)),
        remote(fb.at[t, 15], xe0.at[t], send0.at[4], recv0.at[1 + t], at(1, 0, 0)),
        remote(fb.at[t, 0], xe0.at[t], send0.at[5], recv0.at[1 + t], at(-1, 0, 1)),
        remote(fb.at[t, mine], fb.at[t, mine], send0.at[6], recv0.at[0], at(0, 0, 1 - t)),
        remote(yb0.at[1, 0], y0.at[0, t], send0.at[7], recv0.at[3 + t], at(0, 1, 0)),
        remote(yb0.at[1, 1], y0.at[0, t], send0.at[8], recv0.at[3 + t], at(0, 1, 1)),
        remote(yb0.at[0, 0], y0.at[1, t], send0.at[9], recv0.at[5 + t], at(0, -1, 0)),
        remote(yb0.at[0, 1], y0.at[1, t], send0.at[10], recv0.at[5 + t], at(0, -1, 1)),
    ]
    for copy in first:
        copy.start()

    def ring_signal(sem, axis, reach):
        for step in (reach, -reach):
            dev = at(step, 0, t) if axis == "gx" else at(0, step, t)
            pl.semaphore_signal(sem, inc=1, device_id=dev, device_id_type=MESH)

    hops_x = [h for h in (1, 2, 4, 8) if h < max(nx // 2, 1)]
    hops_y = [h for h in (1, 2, 4, 8) if h < max(ny // 2, 1)]

    def reach_step(i):
        if i > 0:
            if i - 1 < len(hops_x):
                pl.semaphore_wait(far_x.at[i - 1], 2)
            if i - 1 < len(hops_y):
                pl.semaphore_wait(far_y.at[i - 1], 2)
        if i < len(hops_x):
            ring_signal(far_x.at[i], "gx", hops_x[i])
        if i < len(hops_y):
            ring_signal(far_y.at[i], "gy", hops_y[i])

    reach_step(0)

    loads[4].wait()
    loads[5].wait()
    low = lo_s[0]
    high = up_s[0]
    centre = (high + low) / 2.0
    half = (high - low) / 2.0
    rho1 = half / centre
    rho2 = 1.0 / (2.0 * centre / half - rho1)
    first_scale = 1.0 / centre
    keep_scale = rho2 * rho1
    second_scale = 2.0 * rho2 / half

    last_y = ny * 64 - 1
    outer_x = jnp.where(t == 0, gx == 0, gx == nx - 1)
    inner_x = 1.0 - outer_x.astype(F32)
    z_half = jnp.where((lax.rem(lane, 8) == 0) | (lax.rem(lane, 8) == 7), 0.5, 1.0)
    yz_half = z_half * jnp.where((row == 0) | (row == 7), 0.5, 1.0)
    bound = {}
    for h in range(2):
        for e in range(8):
            keep = lane != (127 if h else 0)
            if e == 0:
                keep = keep & ((row + gy * 64) != 0)
            if e == 7:
                keep = keep & ((row + gy * 64 + 56) != last_y)
            bound[h, e] = jnp.where(keep, 1.0, 0.0)
            wn[h, e * 8 : e * 8 + 8, :] = bound[h, e] * yz_half

    def wait_for(dst, sem):
        remote(dst, dst, send0.at[0], sem, at(0, 0, 1 - t)).wait_recv()

    def plane(p):
        return p + t * (15 - 2 * p)

    def y_own(planes):
        for h in range(2):
            for p in planes:
                a = db[h, p, pl.ds(7, 8, stride=8), :]
                b = db[h, p, pl.ds(0, 8, stride=8), :]
                db[h, p, pl.ds(7, 8, stride=8), :] = a + jnp.where(
                    row == 7, 0.0, pltpu.roll(b, 7, 0)
                )
                db[h, p, pl.ds(0, 8, stride=8), :] = b + jnp.where(
                    row == 0, 0.0, pltpu.roll(a, 1, 0)
                )

    def y_add(rows_of):
        low_rows, high_rows = rows_of(0), rows_of(1)
        for h in range(2):
            for p in range(8):
                one = slice(p, p + 1)
                db[h, p, 0:1, :] = db[h, p, 0:1, :] + low_rows[h][one]
                db[h, p, 63:64, :] = db[h, p, 63:64, :] + high_rows[h][one]

    other = 1 - t
    weight_jk = kf[16:24, :]
    wait_for(fb.at[other, theirs], recv0.at[0])
    own_c = [fb[h, plane(0), 64:72, :] for h in range(2)]
    int_c = [fb[h, plane(8), 64:72, :] for h in range(2)]
    for h in range(2):
        for e in range(8):
            cb[h, e * 8 : e * 8 + 8, :] = spread_rows(own_c[h][e : e + 1]) * weight_jk
    for p in range(1, 7):
        db[0, p], db[1, p] = z_sum(fb[0, plane(p), 0:64, :], fb[1, plane(p), 0:64, :])
    y_own(range(1, 7))
    db[0, 7], db[1, 7] = z_sum(
        *[fb[h, plane(7), 0:64, :] + fb[h, plane(8), 0:64, :] for h in range(2)]
    )
    for h in range(2):
        wait_for(xe0.at[h], recv0.at[1 + h])
        for side in range(2):
            wait_for(y0.at[side, h], recv0.at[3 + 2 * side + h])
            wait_for(xy0.at[side, h], recv0.at[7 + 2 * side + h])
    db[0, 0], db[1, 0] = z_sum(
        *[fb[h, plane(0), 0:64, :] + xe0[h, 0:64, :] for h in range(2)]
    )

    def first_rows(side):
        raw = []
        for h in range(2):
            d = y0[side, h, 0:8, :]
            d = d + jnp.where(row == 0, spread_rows(xy0[side, h, 0:1, :]), 0.0)
            d = d + jnp.where(row == 7, spread_rows(y0[side, h, 8:9, :]), 0.0)
            raw.append(d)
        return z_sum(*raw)

    y_own((0, 7))
    y_add(first_rows)

    for variant in range(3):
        own = own_c
        near = [[spread_rows(y0[s, h, 9:10, :]) for h in range(2)] for s in range(2)]
        if variant == 1:
            own = [own[h] + xe0[h, 64:72, :] for h in range(2)]
            near = [
                [near[s][h] + spread_rows(xy0[s, h, 9:10, :]) for h in range(2)] for s in range(2)
            ]
        if variant == 2:
            own = [own[h] + int_c[h] for h in range(2)]
            near = [
                [near[s][h] + spread_rows(y0[s, h, 10:11, :]) for h in range(2)] for s in range(2)
            ]
        own = z_sum(*own)
        near = [z_sum(*pair) for pair in near]
        for h in range(2):
            a = own[h] + jnp.where(row == 7, near[1][h], pltpu.roll(own[h], 7, 0))
            b = own[h] + jnp.where(row == 0, near[0][h], pltpu.roll(own[h], 1, 0))
            for e in range(8):
                one = slice(e, e + 1)
                tile = jnp.where(
                    row == 7,
                    spread_rows(a[one]),
                    jnp.where(row == 0, spread_rows(b[one]), spread_rows(own[h][one])),
                )
                flip = bound[h, e] / tile
                if variant == 1:
                    flip = flip * inner_x
                for p in {0: range(1, 7), 1: (0,), 2: (7,)}[variant]:
                    inv[h, p, e * 8 : e * 8 + 8, :] = flip * kf[24 + 8 * p : 32 + 8 * p, :]

    reach_step(1)
    loads[2].wait()

    stiff = STIFF
    even = [[float(stiff[p, i] + stiff[p, 7 - i]) / 2 for i in range(4)] for p in range(4)]
    odd = [[float(stiff[p, i] - stiff[p, 7 - i]) / 2 for i in range(4)] for p in range(4)]

    def norm_of(acc):
        return jnp.sum(acc)

    regions = {
        "inner": [(p, 16, 32) for p in range(1, 7)],
        "outer": [(0, 0, 64), (7, 0, 64)]
        + [(p, first, 16) for p in range(1, 7) for first in (0, 48)],
    }

    def update(step, region):
        total = jnp.zeros((8, 128), F32)
        for h in range(2):
            for p, first_row, n in regions[region]:
                rows = pl.ds(first_row, n)
                res = db[h, p, rows, :]
                if step > 0:
                    res = r[h, p, rows, :] - res
                if step % 2 == 0:
                    square = res * res * wn[h, rows, :]
                    part = jnp.sum(square.reshape(n // 8, 8, 128), axis=0)
                    if p == 0:
                        part = part * (0.5 * inner_x)
                    if p == 7:
                        part = part * 0.5
                    total = total + part
                if step == ROUNDS:
                    continue
                r[h, p, rows, :] = res
                if step % 2 == 0:
                    new = inv[h, p, rows, :] * (res * first_scale)
                else:
                    new = keep_scale * u[h, p, rows, :] + second_scale * (inv[h, p, rows, :] * res)
                u[h, p, rows, :] = new
                home = p + t * (7 - 2 * p)
                sol[h, home, rows, :] = new if step == 0 else sol[h, home, rows, :] + new
                top = new.astype(BF16)
                uz[h, p, rows, 0:128] = top
                uz[h, p, rows, 128:256] = (new - top.astype(F32)).astype(BF16)
        return total

    def multiply(region):
        along_z = kb[0:256, :]
        many = kb[256:320, 0:192]
        few = kb[320:352, 0:96]
        parts = regions[region]
        for h in range(2):
            lhs = jnp.concatenate([uz[h, p, pl.ds(f, n), :] for p, f, n in parts], axis=0)
            out = jnp.dot(lhs, along_z, preferred_element_type=F32)
            out = out[:, 0:128] + out[:, 128:256]
            at_row = 0
            for p, f, n in parts:
                yz[h, p, pl.ds(f, n), :] = out[at_row : at_row + n]
                at_row += n
        for p in range(8):
            mine_rows = [(f, n) for q, f, n in parts if q == p]
            if not mine_rows:
                continue

            def stack(lanes):
                pieces = [
                    jnp.concatenate(
                        [uz[0, p, pl.ds(f, n), lanes], uz[1, p, pl.ds(f, n), lanes]], axis=1
                    )
                    for f, n in mine_rows
                ]
                return pieces[0] if len(pieces) == 1 else jnp.concatenate(pieces, axis=0)

            top = stack(slice(0, 128))
            both = jnp.concatenate([top, stack(slice(128, 256)), top], axis=0)
            table = many if mine_rows[0][1] == 64 else few
            out = jnp.dot(table, both, preferred_element_type=F32)
            at_row = 0
            for f, n in mine_rows:
                for h in range(2):
                    rows = pl.ds(f, n)
                    piece = out[at_row : at_row + n, h * 128 : h * 128 + 128]
                    yz[h, p, rows, :] = yz[h, p, rows, :] + piece
                at_row += n

    def tile(k, h, e, pairs):
        rows = pl.ds(e * 8, 8)
        val = [u[h, p, rows, :] for p in range(8)]
        plus = [(val[i] + val[7 - i]) for i in range(4)]
        minus = [(val[i] - val[7 - i]) for i in range(4)]
        coef = cb[h, rows, :]
        for p in pairs:
            ev = sum(even[p][i] * plus[i] for i in range(4))
            od = sum(odd[p][i] * minus[i] for i in range(4))
            w = float(WEIGHTS[p])
            d_low = coef * (ev + od + w * yz[h, p, rows, :])
            d_high = coef * (ev - od + w * yz[h, 7 - p, rows, :])
            db[h, p, rows, :] = d_low
            db[h, 7 - p, rows, :] = d_high
            if p == 0:
                sx[k, 0, h, rows, :] = d_low
                sx[k, 1, h, rows, :] = d_high
            if e in (0, 7):
                side = 0 if e == 0 else 1
                j = 0 if e == 0 else 7
                sy[k, side, h, p : p + 1, :] = d_low[j : j + 1]
                sy[k, side, h, 7 - p : 8 - p, :] = d_high[j : j + 1]
                if p == 0:
                    sd[k, 0, side, h : h + 1, :] = d_low[j : j + 1]
                    sd[k, 1, side, h : h + 1, :] = d_high[j : j + 1]

    def messages(k):
        ss = sends.at[k]
        rs = recvs.at[k]
        ext = 2 * t - 1
        return [
            remote(sd.at[k, 0, 0], rd.at[k, 0, 1], ss.at[4], rs.at[5], at(ext, -1, other)),
            remote(sd.at[k, 0, 1], rd.at[k, 0, 0], ss.at[5], rs.at[4], at(ext, 1, other)),
            remote(sx.at[k, 0], rx.at[k, 0], ss.at[0], rs.at[0], at(ext, 0, other)),
            remote(sd.at[k, 1, 0], rd.at[k, 1, 1], ss.at[6], rs.at[7], at(0, -1, other)),
            remote(sd.at[k, 1, 1], rd.at[k, 1, 0], ss.at[7], rs.at[6], at(0, 1, other)),
            remote(sy.at[k, 0], ry.at[k, 1], ss.at[2], rs.at[3], at(0, -1, t)),
            remote(sy.at[k, 1], ry.at[k, 0], ss.at[3], rs.at[2], at(0, 1, t)),
            remote(sx.at[k, 1], rx.at[k, 1], ss.at[1], rs.at[1], at(0, 0, other)),
        ]

    def rows_of_round(k, side):
        raw = []
        for h in range(2):
            d = ry[k, side, h]
            d = d + jnp.where(row == 0, spread_rows(rd[k, 0, side, h : h + 1, :]), 0.0)
            d = d + jnp.where(row == 7, spread_rows(rd[k, 1, side, h : h + 1, :]), 0.0)
            raw.append(d)
        return z_sum(*raw)

    sent = list(first)
    norms = []
    total = update(0, "inner")
    multiply("inner")
    for k in range(ROUNDS):
        total = total + update(k, "outer")
        multiply("outer")
        for h in range(2):
            for e in (0, 7):
                tile(k, h, e, range(4))
            for e in range(1, 7):
                tile(k, h, e, (0,))
        copies = messages(k)
        for copy in copies:
            copy.start()
        sent += copies
        if k % 2 == 0:
            norms.append(norm_of(total))
        if k == ROUNDS - 1:
            half_rows = pl.ds(8 * t, 8)
            away = remote(
                sol.at[other], out_ref.at[half_rows], out_send, out_recv, at(0, 0, other)
            )
            away.start()
            for p in range(8):
                out_ref[8 * t + p] = sol[t, p]
        for h in range(2):
            for e in range(1, 7):
                tile(k, h, e, (1, 2, 3))
        for p in range(1, 7):
            db[0, p], db[1, p] = z_sum(db[0, p], db[1, p])
        y_own(range(1, 7))
        total = update(k + 1, "inner")
        if k < ROUNDS - 1:
            multiply("inner")
        for copy in copies:
            copy.wait_recv()
        for side, p in ((0, 0), (1, 7)):
            db[0, p], db[1, p] = z_sum(db[0, p] + rx[k, side, 0], db[1, p] + rx[k, side, 1])
        y_own((0, 7))
        y_add(lambda side: rows_of_round(k, side))
        reach_step(k + 2)
    norms.append(norm_of(total + update(ROUNDS, "outer")))

    lane1 = lax.broadcasted_iota(jnp.int32, (1, 128), 1)
    line = jnp.where(lane1 == 0, norms[0], jnp.where(lane1 == 1, norms[1], norms[2]))
    v1[...] = line
    hops = []
    for o in range(1, ny):
        hops.append(remote(v1, a1.at[gy], s1_sem.at[o], r1_sem.at[gy], at(0, o, t)))
    for copy in hops:
        copy.start()
    for copy in sent:
        copy.wait_send()
    a1[gy] = line
    for o in range(1, ny):
        source = lax.rem(gy + o, ny)
        wait_for(a1.at[source], r1_sem.at[source])
    line = jnp.sum(a1[...], axis=0)
    v2[...] = line
    slot = gx * 2 + t
    wide = []
    for o in range(0, nx):
        for flip in range(2):
            if o == 0 and flip == 0:
                continue
            core = other if flip else t
            i = 2 * o + flip
            wide.append(remote(v2, a2.at[slot], s2_sem.at[i], r2_sem.at[slot], at(o, 0, core)))
    for copy in wide:
        copy.start()
    for copy in hops + [away]:
        copy.wait_send()
    away.wait_recv()
    a2[slot] = line
    for o in range(0, nx):
        for flip in range(2):
            if o == 0 and flip == 0:
                continue
            source = lax.rem(gx + o, nx) * 2 + (other if flip else t)
            wait_for(a2.at[source], r2_sem.at[source])
    line = jnp.sum(a2[...], axis=0)
    whole = line[0, 0]
    ratios = jnp.sqrt(line / whole)
    ratio_ref[0] = ratios[0, 1]
    ratio_ref[1] = ratios[0, 2]

    for copy in wide:
        copy.wait_send()


def per_device(nx, ny, forcing, conductivity, lower_bound, upper_bound):
    vmem = lambda *shape: pltpu.VMEM(shape, F32)
    dma = lambda *shape: pltpu.SemaphoreType.DMA(shape)
    scratch = [
        vmem(2, 16, 72, 128),
        vmem(2, 72, 128),
        vmem(2, 2, 16, 128),
        vmem(2, 2, 16, 128),
        vmem(2, 2, 16, 128),
        vmem(2, 8, 64, 128),
        vmem(2, 8, 64, 128),
        vmem(2, 8, 64, 128),
        vmem(2, 8, 64, 128),
        vmem(2, 64, 128),
        vmem(2, 64, 128),
        vmem(2, 8, 64, 128),
        pltpu.VMEM((2, 8, 64, 256), BF16),
        vmem(2, 8, 64, 128),
        pltpu.VMEM((352, 256), BF16),
        vmem(88, 128),
        vmem(ROUNDS, 2, 2, 64, 128),
        vmem(ROUNDS, 2, 2, 64, 128),
        vmem(ROUNDS, 2, 2, 8, 128),
        vmem(ROUNDS, 2, 2, 8, 128),
        vmem(ROUNDS, 2, 2, 2, 128),
        vmem(ROUNDS, 2, 2, 2, 128),
        vmem(1, 128),
        vmem(ny, 1, 128),
        vmem(1, 128),
        vmem(2 * nx, 1, 128),
        vmem(2, 8, 16),
        pltpu.SMEM((1,), F32),
        pltpu.SMEM((1,), F32),
        dma(6),
        dma(11),
        dma(11),
        dma(ROUNDS, 8),
        dma(ROUNDS, 8),
        dma(),
        dma(),
        dma(ny),
        dma(ny),
        dma(2 * nx),
        dma(2 * nx),
        pltpu.SemaphoreType.REGULAR((4,)),
        pltpu.SemaphoreType.REGULAR((4,)),
    ]
    anywhere = pl.BlockSpec(memory_space=pl.ANY)
    in_vmem = pl.BlockSpec(memory_space=pltpu.VMEM)
    in_smem = pl.BlockSpec(memory_space=pltpu.SMEM)
    result, line = pl.pallas_call(
        functools.partial(smoother, nx, ny),
        out_shape=(
            pltpu.VMEM(forcing.shape, F32),
            pltpu.SMEM((2,), F32),
        ),
        in_specs=[anywhere] * 6,
        out_specs=(in_vmem, in_smem),
        scratch_shapes=scratch,
        compiler_params=pltpu.CompilerParams(collective_id=0, has_side_effects=True),
    )(
        forcing,
        conductivity,
        lower_bound,
        upper_bound,
        jnp.asarray(bf16_tables(), BF16),
        jnp.asarray(f32_tables(), F32),
    )
    return result, line


def solution(mesh):
    spec = P("gx", "gy", "gz")
    return jax.shard_map(
        functools.partial(per_device, mesh.shape["gx"], mesh.shape["gy"]),
        mesh=mesh,
        in_specs=(spec, spec, P(), P()),
        out_specs=(spec, P()),
        check_vma=False,
    )
```

```python
import functools

import jax
import jax.numpy as jnp
import numpy as np
from jax import lax
from jax.experimental import pallas as pl
from jax.experimental.pallas import tpu as pltpu
from jax.sharding import PartitionSpec as P

MESH = pl.DeviceIdType.MESH
F32 = jnp.float32
BF16 = jnp.bfloat16
ROUNDS = 4

gll_inner = [0.20929921790247888, 0.5917001814331423, 0.8717401485096066]


def gll_tables():
    degree_val = 7
    points = np.array(
        [
            -1.0,
            -gll_inner[2],
            -gll_inner[1],
            -gll_inner[0],
            gll_inner[0],
            gll_inner[1],
            gll_inner[2],
            1.0,
        ]
    )
    previous = np.ones(8)
    values = points * 1.0
    for order in range(1, degree_val):
        following = ((2.0 * order + 1.0) * points * values - order * previous) / (order + 1.0)
        previous = values
        values = following
    weights = 2.0 / (degree_val * (degree_val + 1) * values**2)
    differ = points[:, None] - points[None, :]
    safe_gap = np.where(differ == 0.0, 1.0, differ)
    derivative = np.where(differ == 0.0, 0.0, values[:, None] / values[None, :] / safe_gap)
    corner_val = degree_val * (degree_val + 1) / 4.0
    ends_vec = np.concatenate([np.array([-corner_val]), np.zeros(6), np.array([corner_val])])
    index_row = np.arange(8)
    derivative = derivative + np.where(
        index_row[:, None] == index_row[None, :], ends_vec[None, :], 0.0
    )
    stiffness = derivative.T @ (weights[:, None] * derivative)
    return (weights, stiffness)


WEIGHTS, STIFF = gll_tables()
STIFF = 0.5 * (STIFF + STIFF[::-1, ::-1])
WEIGHTS = 0.5 * (WEIGHTS + WEIGHTS[::-1])


def halves(table):
    high = table.astype(np.float32).astype(jnp.dtype(BF16)).astype(np.float64)
    return high, table - high


def bf16_tables():
    scaled = STIFF / WEIGHTS[:, None]
    wide_z = np.kron(np.eye(16), scaled.T)
    high, low = halves(wide_z)
    along_z = np.block([[high, low], [high, np.zeros_like(low)]])
    wide_y = np.kron(np.eye(8), scaled)
    high, low = halves(wide_y)
    along_y = np.concatenate([high, high, low, np.zeros_like(low)], axis=1)
    few_high, few_low = high[:32, :32], low[:32, :32]
    few = np.concatenate([few_high, few_high, few_low, np.zeros((32, 160))], axis=1)
    return np.concatenate([along_z, along_y, few], axis=0).astype(np.float32)


def f32_tables():
    spread = np.kron(np.eye(16), np.ones((1, 8)))
    w, s = WEIGHTS, np.diagonal(STIFF)
    lanes = lambda v: np.tile(v, 16)[None, :]
    col = lambda v: v[:, None]
    parts = [spread, col(w) * lanes(w)]
    for p in range(8):
        diag = s[p] * col(w) * lanes(w) + w[p] * (col(s) * lanes(w) + col(w) * lanes(s))
        parts.append(1.0 / diag)
    return np.concatenate(parts, axis=0).astype(np.float32)


def smoother(
    nx,
    ny,
    f_ref,
    c_ref,
    lo_ref,
    up_ref,
    kb_ref,
    kf_ref,
    out_ref,
    ratio_ref,
    fb,
    xe0,
    yb0,
    y0,
    xy0,
    u,
    r,
    sol,
    inv,
    cb,
    wn,
    db,
    uz,
    yz,
    kb,
    kf,
    sx,
    rx,
    sy,
    ry,
    sd,
    rd,
    v1,
    a1,
    v2,
    a2,
    cv,
    lo_s,
    up_s,
    load_sem,
    send0,
    recv0,
    sends,
    recvs,
    out_send,
    out_recv,
    s1_sem,
    r1_sem,
    s2_sem,
    r2_sem,
    far_y,
    far_x,
):
    gx = lax.axis_index("gx")
    gy = lax.axis_index("gy")
    t = lax.axis_index("gz")

    def at(dx, dy, core):
        return {"gx": lax.rem(gx + dx + nx, nx), "gy": lax.rem(gy + dy + ny, ny), "gz": core}

    def remote(src, dst, ss, rs, dev):
        return pltpu.make_async_remote_copy(
            src_ref=src, dst_ref=dst, send_sem=ss, recv_sem=rs, device_id=dev, device_id_type=MESH
        )

    barrier = pltpu.get_barrier_semaphore()
    count = 0
    for dx in (-1, 1, 0):
        for dy in (-1, 1, 0):
            for core in (1 - t, t):
                if dx == 0 and dy == 0 and core is t:
                    continue
                pl.semaphore_signal(
                    barrier, inc=1, device_id=at(dx, dy, core), device_id_type=MESH
                )
                count += 1

    loads = [
        pltpu.make_async_copy(f_ref, fb.at[t, :, pl.ds(0, 64)], load_sem.at[0]),
        pltpu.make_async_copy(kf_ref, kf, load_sem.at[1]),
        pltpu.make_async_copy(kb_ref, kb, load_sem.at[2]),
        pltpu.make_async_copy(c_ref, cv, load_sem.at[3]),
        pltpu.make_async_copy(lo_ref, lo_s, load_sem.at[4]),
        pltpu.make_async_copy(up_ref, up_s, load_sem.at[5]),
    ]
    for copy in loads:
        copy.start()

    row = lax.broadcasted_iota(jnp.int32, (8, 128), 0)
    lane = lax.broadcasted_iota(jnp.int32, (8, 128), 1)

    def z_sum(d0, d1):
        at_lane = lax.broadcasted_iota(jnp.int32, d0.shape, 1)
        k = lax.rem(at_lane, 8)
        ends = (k == 0) | (k == 7)
        up = k == 7
        axis = 1
        nxt0 = pltpu.roll(d0, 127, axis)
        nxt1 = pltpu.roll(d1, 127, axis)
        prv0 = pltpu.roll(d0, 1, axis)
        prv1 = pltpu.roll(d1, 1, axis)
        s0 = jnp.where(at_lane == 127, nxt1, jnp.where(up, nxt0, prv0))
        s1 = jnp.where(at_lane == 0, prv0, jnp.where(up, nxt1, prv1))
        zero = jnp.zeros_like(d0)
        return d0 + jnp.where(ends, s0, zero), d1 + jnp.where(ends, s1, zero)

    def spread_rows(value):
        return jnp.broadcast_to(value, (8, 128))

    loads[1].wait()
    loads[3].wait()
    ce = jnp.dot(
        cv[...].reshape(16, 16),
        kf[0:16, :],
        precision=lax.Precision.HIGHEST,
        preferred_element_type=F32,
    )
    for x, e in ((0, 0), (7, 0), (8, 1), (15, 1)):
        fb[t, x, 64:72, :] = ce[e * 8 : e * 8 + 8]
    loads[0].wait()
    for side, y in ((0, 0), (1, 63)):
        for b in range(2):
            for p in range(9):
                x = 15 - p if b else p
                yb0[side, b, p : p + 1, :] = fb[t, x, y : y + 1, :]
            e = 7 * side
            yb0[side, b, 9:10, :] = ce[b * 8 + e : b * 8 + e + 1]
            yb0[side, b, 10:11, :] = ce[(1 - b) * 8 + e : (1 - b) * 8 + e + 1]

    pl.semaphore_wait(barrier, count)

    mine = pl.ds(7 * (1 - t), 9)
    theirs = pl.ds(7 * t, 9)
    first = [
        remote(yb0.at[1, 1], xy0.at[0, t], send0.at[0], recv0.at[7 + t], at(1, 1, 0)),
        remote(yb0.at[0, 1], xy0.at[1, t], send0.at[1], recv0.at[9 + t], at(1, -1, 0)),
        remote(yb0.at[1, 0], xy0.at[0, t], send0.at[2], recv0.at[7 + t], at(-1, 1, 1)),
        remote(yb0.at[0, 0], xy0.at[1, t], send0.at[3], recv0.at[9 + t], at(-1, -1, 1)),
        remote(fb.at[t, 15], xe0.at[t], send0.at[4], recv0.at[1 + t], at(1, 0, 0)),
        remote(fb.at[t, 0], xe0.at[t], send0.at[5], recv0.at[1 + t], at(-1, 0, 1)),
        remote(fb.at[t, mine], fb.at[t, mine], send0.at[6], recv0.at[0], at(0, 0, 1 - t)),
        remote(yb0.at[1, 0], y0.at[0, t], send0.at[7], recv0.at[3 + t], at(0, 1, 0)),
        remote(yb0.at[1, 1], y0.at[0, t], send0.at[8], recv0.at[3 + t], at(0, 1, 1)),
        remote(yb0.at[0, 0], y0.at[1, t], send0.at[9], recv0.at[5 + t], at(0, -1, 0)),
        remote(yb0.at[0, 1], y0.at[1, t], send0.at[10], recv0.at[5 + t], at(0, -1, 1)),
    ]
    for copy in first:
        copy.start()

    def ring_signal(sem, axis, reach):
        for step in (reach, -reach):
            dev = at(step, 0, t) if axis == "gx" else at(0, step, t)
            pl.semaphore_signal(sem, inc=1, device_id=dev, device_id_type=MESH)

    hops_x = [h for h in (1, 2, 4, 8) if h < max(nx // 2, 1)]
    hops_y = [h for h in (1, 2, 4, 8) if h < max(ny // 2, 1)]

    def reach_step(i):
        if i > 0:
            if i - 1 < len(hops_x):
                pl.semaphore_wait(far_x.at[i - 1], 2)
            if i - 1 < len(hops_y):
                pl.semaphore_wait(far_y.at[i - 1], 2)
        if i < len(hops_x):
            ring_signal(far_x.at[i], "gx", hops_x[i])
        if i < len(hops_y):
            ring_signal(far_y.at[i], "gy", hops_y[i])

    reach_step(0)

    loads[4].wait()
    loads[5].wait()
    low = lo_s[0]
    high = up_s[0]
    centre = (high + low) / 2.0
    half = (high - low) / 2.0
    rho1 = half / centre
    rho2 = 1.0 / (2.0 * centre / half - rho1)
    first_scale = 1.0 / centre
    keep_scale = rho2 * rho1
    second_scale = 2.0 * rho2 / half

    last_y = ny * 64 - 1
    outer_x = jnp.where(t == 0, gx == 0, gx == nx - 1)
    inner_x = 1.0 - outer_x.astype(F32)
    z_half = jnp.where((lax.rem(lane, 8) == 0) | (lax.rem(lane, 8) == 7), 0.5, 1.0)
    yz_half = z_half * jnp.where((row == 0) | (row == 7), 0.5, 1.0)
    bound = {}
    for h in range(2):
        for e in range(8):
            keep = lane != (127 if h else 0)
            if e == 0:
                keep = keep & ((row + gy * 64) != 0)
            if e == 7:
                keep = keep & ((row + gy * 64 + 56) != last_y)
            bound[h, e] = jnp.where(keep, 1.0, 0.0)
            wn[h, e * 8 : e * 8 + 8, :] = bound[h, e] * yz_half

    def wait_for(dst, sem):
        remote(dst, dst, send0.at[0], sem, at(0, 0, 1 - t)).wait_recv()

    def plane(p):
        return p + t * (15 - 2 * p)

    def y_own(planes):
        for h in range(2):
            for p in planes:
                a = db[h, p, pl.ds(7, 8, stride=8), :]
                b = db[h, p, pl.ds(0, 8, stride=8), :]
                db[h, p, pl.ds(7, 8, stride=8), :] = a + jnp.where(
                    row == 7, 0.0, pltpu.roll(b, 7, 0)
                )
                db[h, p, pl.ds(0, 8, stride=8), :] = b + jnp.where(
                    row == 0, 0.0, pltpu.roll(a, 1, 0)
                )

    def y_add(rows_of):
        low_rows, high_rows = rows_of(0), rows_of(1)
        for h in range(2):
            for p in range(8):
                one = slice(p, p + 1)
                db[h, p, 0:1, :] = db[h, p, 0:1, :] + low_rows[h][one]
                db[h, p, 63:64, :] = db[h, p, 63:64, :] + high_rows[h][one]

    stiff = STIFF
    even = [[float(stiff[p, i] + stiff[p, 7 - i]) / 2 for i in range(4)] for p in range(4)]
    odd = [[float(stiff[p, i] - stiff[p, 7 - i]) / 2 for i in range(4)] for p in range(4)]

    def norm_of(acc):
        return jnp.sum(acc)

    regions = {
        "inner": [(p, 16, 32) for p in range(1, 7)],
        "outer": [(0, 0, 64), (7, 0, 64)]
        + [(p, first, 16) for p in range(1, 7) for first in (0, 48)],
    }

    def update(step, region):
        total = jnp.zeros((8, 128), F32)
        for h in range(2):
            for p, first_row, n in regions[region]:
                rows = pl.ds(first_row, n)
                res = db[h, p, rows, :]
                if step > 0:
                    res = r[h, p, rows, :] - res
                if step % 2 == 0:
                    square = res * res * wn[h, rows, :]
                    part = jnp.sum(square.reshape(n // 8, 8, 128), axis=0)
                    if p == 0:
                        part = part * (0.5 * inner_x)
                    if p == 7:
                        part = part * 0.5
                    total = total + part
                if step == ROUNDS:
                    continue
                r[h, p, rows, :] = res
                if step % 2 == 0:
                    new = inv[h, p, rows, :] * (res * first_scale)
                else:
                    new = keep_scale * u[h, p, rows, :] + second_scale * (inv[h, p, rows, :] * res)
                u[h, p, rows, :] = new
                home = p + t * (7 - 2 * p)
                sol[h, home, rows, :] = new if step == 0 else sol[h, home, rows, :] + new
                top = new.astype(BF16)
                uz[h, p, rows, 0:128] = top
                uz[h, p, rows, 128:256] = (new - top.astype(F32)).astype(BF16)
        return total

    def multiply(region):
        along_z = kb[0:256, :]
        many = kb[256:320, 0:192]
        few = kb[320:352, 0:96]
        parts = regions[region]
        for h in range(2):
            lhs = jnp.concatenate([uz[h, p, pl.ds(f, n), :] for p, f, n in parts], axis=0)
            out = jnp.dot(lhs, along_z, preferred_element_type=F32)
            out = out[:, 0:128] + out[:, 128:256]
            at_row = 0
            for p, f, n in parts:
                yz[h, p, pl.ds(f, n), :] = out[at_row : at_row + n]
                at_row += n
        for p in range(8):
            mine_rows = [(f, n) for q, f, n in parts if q == p]
            if not mine_rows:
                continue

            def stack(lanes):
                pieces = [
                    jnp.concatenate(
                        [uz[0, p, pl.ds(f, n), lanes], uz[1, p, pl.ds(f, n), lanes]], axis=1
                    )
                    for f, n in mine_rows
                ]
                return pieces[0] if len(pieces) == 1 else jnp.concatenate(pieces, axis=0)

            top = stack(slice(0, 128))
            both = jnp.concatenate([top, stack(slice(128, 256)), top], axis=0)
            table = many if mine_rows[0][1] == 64 else few
            out = jnp.dot(table, both, preferred_element_type=F32)
            at_row = 0
            for f, n in mine_rows:
                for h in range(2):
                    rows = pl.ds(f, n)
                    piece = out[at_row : at_row + n, h * 128 : h * 128 + 128]
                    yz[h, p, rows, :] = yz[h, p, rows, :] + piece
                at_row += n

    def tile(k, h, e, pairs):
        rows = pl.ds(e * 8, 8)
        val = [u[h, p, rows, :] for p in range(8)]
        plus = [(val[i] + val[7 - i]) for i in range(4)]
        minus = [(val[i] - val[7 - i]) for i in range(4)]
        coef = cb[h, rows, :]
        for p in pairs:
            ev = sum(even[p][i] * plus[i] for i in range(4))
            od = sum(odd[p][i] * minus[i] for i in range(4))
            w = float(WEIGHTS[p])
            d_low = coef * (ev + od + w * yz[h, p, rows, :])
            d_high = coef * (ev - od + w * yz[h, 7 - p, rows, :])
            db[h, p, rows, :] = d_low
            db[h, 7 - p, rows, :] = d_high
            if p == 0:
                sx[k, 0, h, rows, :] = d_low
                sx[k, 1, h, rows, :] = d_high
            if e in (0, 7):
                side = 0 if e == 0 else 1
                j = 0 if e == 0 else 7
                sy[k, side, h, p : p + 1, :] = d_low[j : j + 1]
                sy[k, side, h, 7 - p : 8 - p, :] = d_high[j : j + 1]
                if p == 0:
                    sd[k, 0, side, h : h + 1, :] = d_low[j : j + 1]
                    sd[k, 1, side, h : h + 1, :] = d_high[j : j + 1]

    def inverse_tiles(own, near, planes, elements, scale):
        for h in range(2):
            up, down = pltpu.roll(own[h], 7, 0), pltpu.roll(own[h], 1, 0)
            if near is not None:
                up = jnp.where(row == 7, near[1][h], up)
                down = jnp.where(row == 0, near[0][h], down)
            a, b = own[h] + up, own[h] + down
            for e in elements:
                one = slice(e, e + 1)
                ends = jnp.where(
                    row == 0, spread_rows(b[one]), spread_rows(own[h][one])
                )
                flip = bound[h, e] * scale / jnp.where(row == 7, spread_rows(a[one]), ends)
                for p in planes:
                    inv[h, p, e * 8 : e * 8 + 8, :] = flip * kf[24 + 8 * p : 32 + 8 * p, :]

    other = 1 - t
    weight_jk = kf[16:24, :]
    wait_for(fb.at[other, theirs], recv0.at[0])
    own_c = [fb[h, plane(0), 64:72, :] for h in range(2)]
    int_c = [fb[h, plane(8), 64:72, :] for h in range(2)]
    for h in range(2):
        for e in range(8):
            cb[h, e * 8 : e * 8 + 8, :] = spread_rows(own_c[h][e : e + 1]) * weight_jk
    for p in range(1, 7):
        db[0, p], db[1, p] = z_sum(fb[0, plane(p), 0:64, :], fb[1, plane(p), 0:64, :])
    y_own(range(1, 7))
    own_z = z_sum(*own_c)
    inverse_tiles(own_z, None, range(1, 7), range(1, 7), 1.0)
    loads[2].wait()
    total = update(0, "inner")
    multiply("inner")
    db[0, 7], db[1, 7] = z_sum(
        *[fb[h, plane(7), 0:64, :] + fb[h, plane(8), 0:64, :] for h in range(2)]
    )
    for h in range(2):
        wait_for(xe0.at[h], recv0.at[1 + h])
        for side in range(2):
            wait_for(y0.at[side, h], recv0.at[3 + 2 * side + h])
            wait_for(xy0.at[side, h], recv0.at[7 + 2 * side + h])
    db[0, 0], db[1, 0] = z_sum(
        *[fb[h, plane(0), 0:64, :] + xe0[h, 0:64, :] for h in range(2)]
    )

    def first_rows(side):
        raw = []
        for h in range(2):
            d = y0[side, h, 0:8, :]
            d = d + jnp.where(row == 0, spread_rows(xy0[side, h, 0:1, :]), 0.0)
            d = d + jnp.where(row == 7, spread_rows(y0[side, h, 8:9, :]), 0.0)
            raw.append(d)
        return z_sum(*raw)

    y_own((0, 7))
    y_add(first_rows)

    near_c = [[spread_rows(y0[s, h, 9:10, :]) for h in range(2)] for s in range(2)]
    inverse_tiles(own_z, [z_sum(*pair) for pair in near_c], range(1, 7), (0, 7), 1.0)
    ext_near = [
        z_sum(*[near_c[s][h] + spread_rows(xy0[s, h, 9:10, :]) for h in range(2)])
        for s in range(2)
    ]
    ext_own = z_sum(*[own_c[h] + xe0[h, 64:72, :] for h in range(2)])
    inverse_tiles(ext_own, ext_near, (0,), range(8), inner_x)
    int_near = [
        z_sum(*[near_c[s][h] + spread_rows(y0[s, h, 10:11, :]) for h in range(2)])
        for s in range(2)
    ]
    int_own = z_sum(*[own_c[h] + int_c[h] for h in range(2)])
    inverse_tiles(int_own, int_near, (7,), range(8), 1.0)

    def messages(k):
        ss = sends.at[k]
        rs = recvs.at[k]
        ext = 2 * t - 1
        return [
            remote(sd.at[k, 0, 0], rd.at[k, 0, 1], ss.at[4], rs.at[5], at(ext, -1, other)),
            remote(sd.at[k, 0, 1], rd.at[k, 0, 0], ss.at[5], rs.at[4], at(ext, 1, other)),
            remote(sd.at[k, 1, 0], rd.at[k, 1, 1], ss.at[6], rs.at[7], at(0, -1, other)),
            remote(sd.at[k, 1, 1], rd.at[k, 1, 0], ss.at[7], rs.at[6], at(0, 1, other)),
            remote(sy.at[k, 0], ry.at[k, 1], ss.at[2], rs.at[3], at(0, -1, t)),
            remote(sy.at[k, 1], ry.at[k, 0], ss.at[3], rs.at[2], at(0, 1, t)),
            remote(sx.at[k, 0], rx.at[k, 0], ss.at[0], rs.at[0], at(ext, 0, other)),
            remote(sx.at[k, 1], rx.at[k, 1], ss.at[1], rs.at[1], at(0, 0, other)),
        ]

    def rows_of_round(k, side):
        raw = []
        for h in range(2):
            d = ry[k, side, h]
            d = d + jnp.where(row == 0, spread_rows(rd[k, 0, side, h : h + 1, :]), 0.0)
            d = d + jnp.where(row == 7, spread_rows(rd[k, 1, side, h : h + 1, :]), 0.0)
            raw.append(d)
        return z_sum(*raw)

    sent = list(first)
    norms = []
    for k in range(ROUNDS):
        total = total + update(k, "outer")
        multiply("outer")
        copies = messages(k)
        for h in range(2):
            for e in (0, 7):
                tile(k, h, e, range(4))
        for copy in copies[:6]:
            copy.start()
        for h in range(2):
            for e in range(1, 7):
                tile(k, h, e, (0,))
        for copy in copies[6:]:
            copy.start()
        sent += copies
        reach_step(k + 1)
        if k % 2 == 0:
            norms.append(norm_of(total))
        if k == ROUNDS - 1:
            half_rows = pl.ds(8 * t, 8)
            away = remote(
                sol.at[other], out_ref.at[half_rows], out_send, out_recv, at(0, 0, other)
            )
            away.start()
            for p in range(8):
                out_ref[8 * t + p] = sol[t, p]
        for h in range(2):
            for e in range(1, 7):
                tile(k, h, e, (1, 2, 3))
        for p in range(1, 7):
            db[0, p], db[1, p] = z_sum(db[0, p], db[1, p])
        y_own(range(1, 7))
        total = update(k + 1, "inner")
        if k < ROUNDS - 1:
            multiply("inner")
        for copy in copies:
            copy.wait_recv()
        for side, p in ((0, 0), (1, 7)):
            db[0, p], db[1, p] = z_sum(db[0, p] + rx[k, side, 0], db[1, p] + rx[k, side, 1])
        y_own((0, 7))
        y_add(lambda side: rows_of_round(k, side))
    norms.append(norm_of(total + update(ROUNDS, "outer")))

    lane1 = lax.broadcasted_iota(jnp.int32, (1, 128), 1)
    line = jnp.where(lane1 == 0, norms[0], jnp.where(lane1 == 1, norms[1], norms[2]))
    v1[...] = line
    hops = []
    for o in sorted(range(1, ny), key=lambda o: -min(o, ny - o)):
        hops.append(remote(v1, a1.at[gy], s1_sem.at[o], r1_sem.at[gy], at(0, o, t)))
    for copy in hops:
        copy.start()
    for copy in sent:
        copy.wait_send()
    a1[gy] = line
    for o in range(1, ny):
        source = lax.rem(gy + o, ny)
        wait_for(a1.at[source], r1_sem.at[source])
    line = jnp.sum(a1[...], axis=0)
    v2[...] = line
    slot = gx * 2 + t
    wide = []
    for o in range(0, nx):
        for flip in range(2):
            if o == 0 and flip == 0:
                continue
            core = other if flip else t
            i = 2 * o + flip
            wide.append(remote(v2, a2.at[slot], s2_sem.at[i], r2_sem.at[slot], at(o, 0, core)))
    for copy in wide:
        copy.start()
    for copy in hops + [away]:
        copy.wait_send()
    away.wait_recv()
    a2[slot] = line
    for o in range(0, nx):
        for flip in range(2):
            if o == 0 and flip == 0:
                continue
            source = lax.rem(gx + o, nx) * 2 + (other if flip else t)
            wait_for(a2.at[source], r2_sem.at[source])
    line = jnp.sum(a2[...], axis=0)
    whole = line[0, 0]
    ratios = jnp.sqrt(line / whole)
    ratio_ref[0] = ratios[0, 1]
    ratio_ref[1] = ratios[0, 2]

    for copy in wide:
        copy.wait_send()


def per_device(nx, ny, forcing, conductivity, lower_bound, upper_bound):
    vmem = lambda *shape: pltpu.VMEM(shape, F32)
    dma = lambda *shape: pltpu.SemaphoreType.DMA(shape)
    scratch = [
        vmem(2, 16, 72, 128),
        vmem(2, 72, 128),
        vmem(2, 2, 16, 128),
        vmem(2, 2, 16, 128),
        vmem(2, 2, 16, 128),
        vmem(2, 8, 64, 128),
        vmem(2, 8, 64, 128),
        vmem(2, 8, 64, 128),
        vmem(2, 8, 64, 128),
        vmem(2, 64, 128),
        vmem(2, 64, 128),
        vmem(2, 8, 64, 128),
        pltpu.VMEM((2, 8, 64, 256), BF16),
        vmem(2, 8, 64, 128),
        pltpu.VMEM((352, 256), BF16),
        vmem(88, 128),
        vmem(ROUNDS, 2, 2, 64, 128),
        vmem(ROUNDS, 2, 2, 64, 128),
        vmem(ROUNDS, 2, 2, 8, 128),
        vmem(ROUNDS, 2, 2, 8, 128),
        vmem(ROUNDS, 2, 2, 2, 128),
        vmem(ROUNDS, 2, 2, 2, 128),
        vmem(1, 128),
        vmem(ny, 1, 128),
        vmem(1, 128),
        vmem(2 * nx, 1, 128),
        vmem(2, 8, 16),
        pltpu.SMEM((1,), F32),
        pltpu.SMEM((1,), F32),
        dma(6),
        dma(11),
        dma(11),
        dma(ROUNDS, 8),
        dma(ROUNDS, 8),
        dma(),
        dma(),
        dma(ny),
        dma(ny),
        dma(2 * nx),
        dma(2 * nx),
        pltpu.SemaphoreType.REGULAR((4,)),
        pltpu.SemaphoreType.REGULAR((4,)),
    ]
    anywhere = pl.BlockSpec(memory_space=pl.ANY)
    in_vmem = pl.BlockSpec(memory_space=pltpu.VMEM)
    in_smem = pl.BlockSpec(memory_space=pltpu.SMEM)
    result, line = pl.pallas_call(
        functools.partial(smoother, nx, ny),
        out_shape=(
            pltpu.VMEM(forcing.shape, F32),
            pltpu.SMEM((2,), F32),
        ),
        in_specs=[anywhere] * 6,
        out_specs=(in_vmem, in_smem),
        scratch_shapes=scratch,
        compiler_params=pltpu.CompilerParams(collective_id=0, has_side_effects=True),
    )(
        forcing,
        conductivity,
        lower_bound,
        upper_bound,
        jnp.asarray(bf16_tables(), BF16),
        jnp.asarray(f32_tables(), F32),
    )
    return result, line


def solution(mesh):
    spec = P("gx", "gy", "gz")
    return jax.shard_map(
        functools.partial(per_device, mesh.shape["gx"], mesh.shape["gy"]),
        mesh=mesh,
        in_specs=(spec, spec, P(), P()),
        out_specs=(spec, P()),
        check_vma=False,
    )
```

```python
import functools

import jax
import jax.numpy as jnp
import numpy as np
from jax import lax
from jax.experimental import pallas as pl
from jax.experimental.pallas import tpu as pltpu
from jax.sharding import PartitionSpec as P

MESH = pl.DeviceIdType.MESH
F32 = jnp.float32
BF16 = jnp.bfloat16
ROUNDS = 4

gll_inner = [0.20929921790247888, 0.5917001814331423, 0.8717401485096066]


def gll_tables():
    degree_val = 7
    points = np.array(
        [
            -1.0,
            -gll_inner[2],
            -gll_inner[1],
            -gll_inner[0],
            gll_inner[0],
            gll_inner[1],
            gll_inner[2],
            1.0,
        ]
    )
    previous = np.ones(8)
    values = points * 1.0
    for order in range(1, degree_val):
        following = ((2.0 * order + 1.0) * points * values - order * previous) / (order + 1.0)
        previous = values
        values = following
    weights = 2.0 / (degree_val * (degree_val + 1) * values**2)
    differ = points[:, None] - points[None, :]
    safe_gap = np.where(differ == 0.0, 1.0, differ)
    derivative = np.where(differ == 0.0, 0.0, values[:, None] / values[None, :] / safe_gap)
    corner_val = degree_val * (degree_val + 1) / 4.0
    ends_vec = np.concatenate([np.array([-corner_val]), np.zeros(6), np.array([corner_val])])
    index_row = np.arange(8)
    derivative = derivative + np.where(
        index_row[:, None] == index_row[None, :], ends_vec[None, :], 0.0
    )
    stiffness = derivative.T @ (weights[:, None] * derivative)
    return (weights, stiffness)


WEIGHTS, STIFF = gll_tables()
STIFF = 0.5 * (STIFF + STIFF[::-1, ::-1])
WEIGHTS = 0.5 * (WEIGHTS + WEIGHTS[::-1])


def halves(table):
    high = table.astype(np.float32).astype(jnp.dtype(BF16)).astype(np.float64)
    return high, table - high


def bf16_tables():
    scaled = STIFF / WEIGHTS[:, None]
    wide_z = np.kron(np.eye(16), scaled.T)
    high, low = halves(wide_z)
    along_z = np.block([[high, low], [high, np.zeros_like(low)]])
    wide_y = np.kron(np.eye(8), scaled)
    high, low = halves(wide_y)
    along_y = np.concatenate([high, high, low, np.zeros_like(low)], axis=1)
    few_high, few_low = high[:32, :32], low[:32, :32]
    few = np.concatenate([few_high, few_high, few_low, np.zeros((32, 160))], axis=1)
    return np.concatenate([along_z, along_y, few], axis=0).astype(np.float32)


def f32_tables():
    spread = np.kron(np.eye(16), np.ones((1, 8)))
    w, s = WEIGHTS, np.diagonal(STIFF)
    lanes = lambda v: np.tile(v, 16)[None, :]
    col = lambda v: v[:, None]
    parts = [spread, col(w) * lanes(w)]
    for p in range(8):
        diag = s[p] * col(w) * lanes(w) + w[p] * (col(s) * lanes(w) + col(w) * lanes(s))
        parts.append(1.0 / diag)
    return np.concatenate(parts, axis=0).astype(np.float32)


def smoother(
    nx,
    ny,
    f_ref,
    c_ref,
    lo_ref,
    up_ref,
    kb_ref,
    kf_ref,
    out_ref,
    ratio_ref,
    fb,
    xe0,
    yb0,
    y0,
    xy0,
    u,
    r,
    sol,
    inv,
    cb,
    wn,
    db,
    uz,
    yz,
    kb,
    kf,
    sx,
    rx,
    sy,
    ry,
    sd,
    rd,
    v1,
    a1,
    v2,
    a2,
    cv,
    lo_s,
    up_s,
    load_sem,
    send0,
    recv0,
    sends,
    recvs,
    out_send,
    out_recv,
    s1_sem,
    r1_sem,
    s2_sem,
    r2_sem,
    far_y,
    far_x,
):
    gx = lax.axis_index("gx")
    gy = lax.axis_index("gy")
    t = lax.axis_index("gz")

    def at(dx, dy, core):
        return {"gx": lax.rem(gx + dx + nx, nx), "gy": lax.rem(gy + dy + ny, ny), "gz": core}

    def remote(src, dst, ss, rs, dev):
        return pltpu.make_async_remote_copy(
            src_ref=src, dst_ref=dst, send_sem=ss, recv_sem=rs, device_id=dev, device_id_type=MESH
        )

    barrier = pltpu.get_barrier_semaphore()
    count = 0
    for dx in (-1, 1, 0):
        for dy in (-1, 1, 0):
            for core in (1 - t, t):
                if dx == 0 and dy == 0 and core is t:
                    continue
                pl.semaphore_signal(
                    barrier, inc=1, device_id=at(dx, dy, core), device_id_type=MESH
                )
                count += 1

    loads = [
        pltpu.make_async_copy(f_ref, fb.at[t, :, pl.ds(0, 64)], load_sem.at[0]),
        pltpu.make_async_copy(kf_ref, kf, load_sem.at[1]),
        pltpu.make_async_copy(kb_ref, kb, load_sem.at[2]),
        pltpu.make_async_copy(c_ref, cv, load_sem.at[3]),
        pltpu.make_async_copy(lo_ref, lo_s, load_sem.at[4]),
        pltpu.make_async_copy(up_ref, up_s, load_sem.at[5]),
    ]
    for copy in loads:
        copy.start()

    row = lax.broadcasted_iota(jnp.int32, (8, 128), 0)
    lane = lax.broadcasted_iota(jnp.int32, (8, 128), 1)

    def z_sum(d0, d1):
        at_lane = lax.broadcasted_iota(jnp.int32, d0.shape, 1)
        k = lax.rem(at_lane, 8)
        ends = (k == 0) | (k == 7)
        up = k == 7
        axis = 1
        nxt0 = pltpu.roll(d0, 127, axis)
        nxt1 = pltpu.roll(d1, 127, axis)
        prv0 = pltpu.roll(d0, 1, axis)
        prv1 = pltpu.roll(d1, 1, axis)
        s0 = jnp.where(at_lane == 127, nxt1, jnp.where(up, nxt0, prv0))
        s1 = jnp.where(at_lane == 0, prv0, jnp.where(up, nxt1, prv1))
        zero = jnp.zeros_like(d0)
        return d0 + jnp.where(ends, s0, zero), d1 + jnp.where(ends, s1, zero)

    def spread_rows(value):
        return jnp.broadcast_to(value, (8, 128))

    loads[1].wait()
    loads[3].wait()
    ce = jnp.dot(
        cv[...].reshape(16, 16),
        kf[0:16, :],
        precision=lax.Precision.HIGHEST,
        preferred_element_type=F32,
    )
    for x, e in ((0, 0), (7, 0), (8, 1), (15, 1)):
        fb[t, x, 64:72, :] = ce[e * 8 : e * 8 + 8]
    loads[0].wait()
    for side, y in ((0, 0), (1, 63)):
        for b in range(2):
            for p in range(9):
                x = 15 - p if b else p
                yb0[side, b, p : p + 1, :] = fb[t, x, y : y + 1, :]
            e = 7 * side
            yb0[side, b, 9:10, :] = ce[b * 8 + e : b * 8 + e + 1]
            yb0[side, b, 10:11, :] = ce[(1 - b) * 8 + e : (1 - b) * 8 + e + 1]

    pl.semaphore_wait(barrier, count)

    mine = pl.ds(7 * (1 - t), 9)
    theirs = pl.ds(7 * t, 9)
    first = [
        remote(yb0.at[1, 1], xy0.at[0, t], send0.at[0], recv0.at[7 + t], at(1, 1, 0)),
        remote(yb0.at[0, 1], xy0.at[1, t], send0.at[1], recv0.at[9 + t], at(1, -1, 0)),
        remote(yb0.at[1, 0], xy0.at[0, t], send0.at[2], recv0.at[7 + t], at(-1, 1, 1)),
        remote(yb0.at[0, 0], xy0.at[1, t], send0.at[3], recv0.at[9 + t], at(-1, -1, 1)),
        remote(fb.at[t, 15], xe0.at[t], send0.at[4], recv0.at[1 + t], at(1, 0, 0)),
        remote(fb.at[t, 0], xe0.at[t], send0.at[5], recv0.at[1 + t], at(-1, 0, 1)),
        remote(fb.at[t, mine], fb.at[t, mine], send0.at[6], recv0.at[0], at(0, 0, 1 - t)),
        remote(yb0.at[1, 0], y0.at[0, t], send0.at[7], recv0.at[3 + t], at(0, 1, 0)),
        remote(yb0.at[1, 1], y0.at[0, t], send0.at[8], recv0.at[3 + t], at(0, 1, 1)),
        remote(yb0.at[0, 0], y0.at[1, t], send0.at[9], recv0.at[5 + t], at(0, -1, 0)),
        remote(yb0.at[0, 1], y0.at[1, t], send0.at[10], recv0.at[5 + t], at(0, -1, 1)),
    ]
    for copy in first:
        copy.start()

    def ring_signal(sem, axis, reach):
        for step in (reach, -reach):
            dev = at(step, 0, t) if axis == "gx" else at(0, step, t)
            pl.semaphore_signal(sem, inc=1, device_id=dev, device_id_type=MESH)

    hops_x = [h for h in (1, 2, 4, 8) if h < max(nx // 2, 1)]
    hops_y = [h for h in (1, 2, 4, 8) if h < max(ny // 2, 1)]

    def reach_step(i):
        if i > 0:
            if i - 1 < len(hops_x):
                pl.semaphore_wait(far_x.at[i - 1], 2)
            if i - 1 < len(hops_y):
                pl.semaphore_wait(far_y.at[i - 1], 2)
        if i < len(hops_x):
            ring_signal(far_x.at[i], "gx", hops_x[i])
        if i < len(hops_y):
            ring_signal(far_y.at[i], "gy", hops_y[i])

    reach_step(0)

    loads[4].wait()
    loads[5].wait()
    low = lo_s[0]
    high = up_s[0]
    centre = (high + low) / 2.0
    half = (high - low) / 2.0
    rho1 = half / centre
    rho2 = 1.0 / (2.0 * centre / half - rho1)
    first_scale = 1.0 / centre
    keep_scale = rho2 * rho1
    second_scale = 2.0 * rho2 / half

    last_y = ny * 64 - 1
    outer_x = jnp.where(t == 0, gx == 0, gx == nx - 1)
    inner_x = 1.0 - outer_x.astype(F32)
    z_half = jnp.where((lax.rem(lane, 8) == 0) | (lax.rem(lane, 8) == 7), 0.5, 1.0)
    yz_half = z_half * jnp.where((row == 0) | (row == 7), 0.5, 1.0)
    bound = {}
    for h in range(2):
        for e in range(8):
            keep = lane != (127 if h else 0)
            if e == 0:
                keep = keep & ((row + gy * 64) != 0)
            if e == 7:
                keep = keep & ((row + gy * 64 + 56) != last_y)
            bound[h, e] = jnp.where(keep, 1.0, 0.0)
            wn[h, e * 8 : e * 8 + 8, :] = bound[h, e] * yz_half

    def wait_for(dst, sem):
        remote(dst, dst, send0.at[0], sem, at(0, 0, 1 - t)).wait_recv()

    def plane(p):
        return p + t * (15 - 2 * p)

    def y_own(planes):
        for h in range(2):
            for p in planes:
                a = db[h, p, pl.ds(7, 8, stride=8), :]
                b = db[h, p, pl.ds(0, 8, stride=8), :]
                db[h, p, pl.ds(7, 8, stride=8), :] = a + jnp.where(
                    row == 7, 0.0, pltpu.roll(b, 7, 0)
                )
                db[h, p, pl.ds(0, 8, stride=8), :] = b + jnp.where(
                    row == 0, 0.0, pltpu.roll(a, 1, 0)
                )

    def y_add(rows_of):
        low_rows, high_rows = rows_of(0), rows_of(1)
        for h in range(2):
            for p in range(8):
                one = slice(p, p + 1)
                db[h, p, 0:1, :] = db[h, p, 0:1, :] + low_rows[h][one]
                db[h, p, 63:64, :] = db[h, p, 63:64, :] + high_rows[h][one]

    stiff = STIFF
    even = [[float(stiff[p, i] + stiff[p, 7 - i]) / 2 for i in range(4)] for p in range(4)]
    odd = [[float(stiff[p, i] - stiff[p, 7 - i]) / 2 for i in range(4)] for p in range(4)]

    def norm_of(acc):
        return jnp.sum(acc)

    regions = {
        "inner": [(p, 16, 32) for p in range(1, 7)],
        "outer": [(0, 0, 64), (7, 0, 64)]
        + [(p, first, 16) for p in range(1, 7) for first in (0, 48)],
    }

    def square_of(res, h, p, rows, n):
        square = res * res * wn[h, rows, :]
        part = jnp.sum(square.reshape(n // 8, 8, 128), axis=0)
        if p == 0:
            part = part * (0.5 * inner_x)
        if p == 7:
            part = part * 0.5
        return part

    def update(step, region):
        total = jnp.zeros((8, 128), F32)
        for h in range(2):
            for p, first_row, n in regions[region]:
                rows = pl.ds(first_row, n)
                res = db[h, p, rows, :]
                if step > 0:
                    res = r[h, p, rows, :] - res
                if step == ROUNDS or (step % 2 == 0 and region == "inner"):
                    total = total + square_of(res, h, p, rows, n)
                if step == ROUNDS:
                    continue
                r[h, p, rows, :] = res
                if step % 2 == 0:
                    new = inv[h, p, rows, :] * (res * first_scale)
                else:
                    new = keep_scale * u[h, p, rows, :] + second_scale * (inv[h, p, rows, :] * res)
                u[h, p, rows, :] = new
                home = p + t * (7 - 2 * p)
                sol[h, home, rows, :] = new if step == 0 else sol[h, home, rows, :] + new
                top = new.astype(BF16)
                uz[h, p, rows, 0:128] = top
                uz[h, p, rows, 128:256] = (new - top.astype(F32)).astype(BF16)
        return total

    def multiply(region):
        along_z = kb[0:256, :]
        many = kb[256:320, 0:192]
        few = kb[320:352, 0:96]
        parts = regions[region]
        for h in range(2):
            lhs = jnp.concatenate([uz[h, p, pl.ds(f, n), :] for p, f, n in parts], axis=0)
            out = jnp.dot(lhs, along_z, preferred_element_type=F32)
            out = out[:, 0:128] + out[:, 128:256]
            at_row = 0
            for p, f, n in parts:
                yz[h, p, pl.ds(f, n), :] = out[at_row : at_row + n]
                at_row += n
        for p in range(8):
            mine_rows = [(f, n) for q, f, n in parts if q == p]
            if not mine_rows:
                continue

            def stack(lanes):
                pieces = [
                    jnp.concatenate(
                        [uz[0, p, pl.ds(f, n), lanes], uz[1, p, pl.ds(f, n), lanes]], axis=1
                    )
                    for f, n in mine_rows
                ]
                return pieces[0] if len(pieces) == 1 else jnp.concatenate(pieces, axis=0)

            top = stack(slice(0, 128))
            both = jnp.concatenate([top, stack(slice(128, 256)), top], axis=0)
            table = many if mine_rows[0][1] == 64 else few
            out = jnp.dot(table, both, preferred_element_type=F32)
            at_row = 0
            for f, n in mine_rows:
                for h in range(2):
                    rows = pl.ds(f, n)
                    piece = out[at_row : at_row + n, h * 128 : h * 128 + 128]
                    yz[h, p, rows, :] = yz[h, p, rows, :] + piece
                at_row += n

    def tile(k, h, e, pairs):
        rows = pl.ds(e * 8, 8)
        val = [u[h, p, rows, :] for p in range(8)]
        plus = [(val[i] + val[7 - i]) for i in range(4)]
        minus = [(val[i] - val[7 - i]) for i in range(4)]
        coef = cb[h, rows, :]
        for p in pairs:
            ev = sum(even[p][i] * plus[i] for i in range(4))
            od = sum(odd[p][i] * minus[i] for i in range(4))
            w = float(WEIGHTS[p])
            d_low = coef * (ev + od + w * yz[h, p, rows, :])
            d_high = coef * (ev - od + w * yz[h, 7 - p, rows, :])
            db[h, p, rows, :] = d_low
            db[h, 7 - p, rows, :] = d_high
            if p == 0:
                sx[k, 0, h, rows, :] = d_low
                sx[k, 1, h, rows, :] = d_high
            if e in (0, 7):
                side = 0 if e == 0 else 1
                j = 0 if e == 0 else 7
                sy[k, side, h, p : p + 1, :] = d_low[j : j + 1]
                sy[k, side, h, 7 - p : 8 - p, :] = d_high[j : j + 1]
                if p == 0:
                    sd[k, 0, side, h : h + 1, :] = d_low[j : j + 1]
                    sd[k, 1, side, h : h + 1, :] = d_high[j : j + 1]

    def inverse_tiles(own, near, planes, elements, scale):
        for h in range(2):
            up, down = pltpu.roll(own[h], 7, 0), pltpu.roll(own[h], 1, 0)
            if near is not None:
                up = jnp.where(row == 7, near[1][h], up)
                down = jnp.where(row == 0, near[0][h], down)
            a, b = own[h] + up, own[h] + down
            for e in elements:
                one = slice(e, e + 1)
                ends = jnp.where(
                    row == 0, spread_rows(b[one]), spread_rows(own[h][one])
                )
                flip = bound[h, e] * scale / jnp.where(row == 7, spread_rows(a[one]), ends)
                for p in planes:
                    inv[h, p, e * 8 : e * 8 + 8, :] = flip * kf[24 + 8 * p : 32 + 8 * p, :]

    other = 1 - t
    weight_jk = kf[16:24, :]
    wait_for(fb.at[other, theirs], recv0.at[0])
    own_c = [fb[h, plane(0), 64:72, :] for h in range(2)]
    int_c = [fb[h, plane(8), 64:72, :] for h in range(2)]
    for h in range(2):
        for e in range(8):
            cb[h, e * 8 : e * 8 + 8, :] = spread_rows(own_c[h][e : e + 1]) * weight_jk
    for p in range(1, 7):
        db[0, p], db[1, p] = z_sum(fb[0, plane(p), 0:64, :], fb[1, plane(p), 0:64, :])
    y_own(range(1, 7))
    own_z = z_sum(*own_c)
    inverse_tiles(own_z, None, range(1, 7), range(1, 7), 1.0)
    loads[2].wait()
    total = update(0, "inner")
    multiply("inner")
    db[0, 7], db[1, 7] = z_sum(
        *[fb[h, plane(7), 0:64, :] + fb[h, plane(8), 0:64, :] for h in range(2)]
    )
    for h in range(2):
        wait_for(xe0.at[h], recv0.at[1 + h])
        for side in range(2):
            wait_for(y0.at[side, h], recv0.at[3 + 2 * side + h])
            wait_for(xy0.at[side, h], recv0.at[7 + 2 * side + h])
    db[0, 0], db[1, 0] = z_sum(
        *[fb[h, plane(0), 0:64, :] + xe0[h, 0:64, :] for h in range(2)]
    )

    def first_rows(side):
        raw = []
        for h in range(2):
            d = y0[side, h, 0:8, :]
            d = d + jnp.where(row == 0, spread_rows(xy0[side, h, 0:1, :]), 0.0)
            d = d + jnp.where(row == 7, spread_rows(y0[side, h, 8:9, :]), 0.0)
            raw.append(d)
        return z_sum(*raw)

    y_own((0, 7))
    y_add(first_rows)

    near_c = [[spread_rows(y0[s, h, 9:10, :]) for h in range(2)] for s in range(2)]
    inverse_tiles(own_z, [z_sum(*pair) for pair in near_c], range(1, 7), (0, 7), 1.0)
    ext_near = [
        z_sum(*[near_c[s][h] + spread_rows(xy0[s, h, 9:10, :]) for h in range(2)])
        for s in range(2)
    ]
    ext_own = z_sum(*[own_c[h] + xe0[h, 64:72, :] for h in range(2)])
    inverse_tiles(ext_own, ext_near, (0,), range(8), inner_x)
    int_near = [
        z_sum(*[near_c[s][h] + spread_rows(y0[s, h, 10:11, :]) for h in range(2)])
        for s in range(2)
    ]
    int_own = z_sum(*[own_c[h] + int_c[h] for h in range(2)])
    inverse_tiles(int_own, int_near, (7,), range(8), 1.0)

    def messages(k):
        ss = sends.at[k]
        rs = recvs.at[k]
        ext = 2 * t - 1
        return [
            remote(sd.at[k, 0, 0], rd.at[k, 0, 1], ss.at[4], rs.at[5], at(ext, -1, other)),
            remote(sd.at[k, 0, 1], rd.at[k, 0, 0], ss.at[5], rs.at[4], at(ext, 1, other)),
            remote(sd.at[k, 1, 0], rd.at[k, 1, 1], ss.at[6], rs.at[7], at(0, -1, other)),
            remote(sd.at[k, 1, 1], rd.at[k, 1, 0], ss.at[7], rs.at[6], at(0, 1, other)),
            remote(sy.at[k, 0], ry.at[k, 1], ss.at[2], rs.at[3], at(0, -1, t)),
            remote(sy.at[k, 1], ry.at[k, 0], ss.at[3], rs.at[2], at(0, 1, t)),
            remote(sx.at[k, 0], rx.at[k, 0], ss.at[0], rs.at[0], at(ext, 0, other)),
            remote(sx.at[k, 1], rx.at[k, 1], ss.at[1], rs.at[1], at(0, 0, other)),
        ]

    def rows_of_round(k, side):
        raw = []
        for h in range(2):
            d = ry[k, side, h]
            d = d + jnp.where(row == 0, spread_rows(rd[k, 0, side, h : h + 1, :]), 0.0)
            d = d + jnp.where(row == 7, spread_rows(rd[k, 1, side, h : h + 1, :]), 0.0)
            raw.append(d)
        return z_sum(*raw)

    sent = list(first)
    norms = []
    for k in range(ROUNDS):
        total = total + update(k, "outer")
        multiply("outer")
        copies = messages(k)
        for h in range(2):
            for e in (0, 7):
                tile(k, h, e, range(4))
        for copy in copies[:6]:
            copy.start()
        for h in range(2):
            for e in range(1, 7):
                tile(k, h, e, (0,))
        for copy in copies[6:]:
            copy.start()
        sent += copies
        reach_step(k + 1)
        if k % 2 == 0:
            for h in range(2):
                for p, first_row, n in regions["outer"]:
                    rows = pl.ds(first_row, n)
                    total = total + square_of(r[h, p, rows, :], h, p, rows, n)
            norms.append(norm_of(total))
        if k == ROUNDS - 1:
            half_rows = pl.ds(8 * t, 8)
            away = remote(
                sol.at[other], out_ref.at[half_rows], out_send, out_recv, at(0, 0, other)
            )
            away.start()
            for p in range(8):
                out_ref[8 * t + p] = sol[t, p]
        for h in range(2):
            for e in range(1, 7):
                tile(k, h, e, (1, 2, 3))
        for p in range(1, 7):
            db[0, p], db[1, p] = z_sum(db[0, p], db[1, p])
        y_own(range(1, 7))
        total = update(k + 1, "inner")
        if k < ROUNDS - 1:
            multiply("inner")
        for copy in copies:
            copy.wait_recv()
        for side, p in ((0, 0), (1, 7)):
            db[0, p], db[1, p] = z_sum(db[0, p] + rx[k, side, 0], db[1, p] + rx[k, side, 1])
        y_own((0, 7))
        y_add(lambda side: rows_of_round(k, side))
    norms.append(norm_of(total + update(ROUNDS, "outer")))

    lane1 = lax.broadcasted_iota(jnp.int32, (1, 128), 1)
    line = jnp.where(lane1 == 0, norms[0], jnp.where(lane1 == 1, norms[1], norms[2]))
    v1[...] = line
    hops = []
    for o in sorted(range(1, ny), key=lambda o: -min(o, ny - o)):
        hops.append(remote(v1, a1.at[gy], s1_sem.at[o], r1_sem.at[gy], at(0, o, t)))
    for copy in hops:
        copy.start()
    for copy in sent:
        copy.wait_send()
    a1[gy] = line
    for o in range(1, ny):
        source = lax.rem(gy + o, ny)
        wait_for(a1.at[source], r1_sem.at[source])
    line = jnp.sum(a1[...], axis=0)
    v2[...] = line
    slot = gx * 2 + t
    wide = []
    far_first = sorted(
        range(nx), key=lambda o: -min(o % 4, 4 - o % 4) - min(o // 4, 4 - o // 4)
    )
    for o in far_first:
        for flip in (1, 0):
            if o == 0 and flip == 0:
                continue
            core = other if flip else t
            i = 2 * o + flip
            wide.append(remote(v2, a2.at[slot], s2_sem.at[i], r2_sem.at[slot], at(o, 0, core)))
    for copy in wide:
        copy.start()
    for copy in hops + [away]:
        copy.wait_send()
    away.wait_recv()
    a2[slot] = line
    for o in range(0, nx):
        for flip in range(2):
            if o == 0 and flip == 0:
                continue
            source = lax.rem(gx + o, nx) * 2 + (other if flip else t)
            wait_for(a2.at[source], r2_sem.at[source])
    line = jnp.sum(a2[...], axis=0)
    whole = line[0, 0]
    ratios = jnp.sqrt(line / whole)
    ratio_ref[0] = ratios[0, 1]
    ratio_ref[1] = ratios[0, 2]

    for copy in wide:
        copy.wait_send()


def per_device(nx, ny, forcing, conductivity, lower_bound, upper_bound):
    vmem = lambda *shape: pltpu.VMEM(shape, F32)
    dma = lambda *shape: pltpu.SemaphoreType.DMA(shape)
    scratch = [
        vmem(2, 16, 72, 128),
        vmem(2, 72, 128),
        vmem(2, 2, 16, 128),
        vmem(2, 2, 16, 128),
        vmem(2, 2, 16, 128),
        vmem(2, 8, 64, 128),
        vmem(2, 8, 64, 128),
        vmem(2, 8, 64, 128),
        vmem(2, 8, 64, 128),
        vmem(2, 64, 128),
        vmem(2, 64, 128),
        vmem(2, 8, 64, 128),
        pltpu.VMEM((2, 8, 64, 256), BF16),
        vmem(2, 8, 64, 128),
        pltpu.VMEM((352, 256), BF16),
        vmem(88, 128),
        vmem(ROUNDS, 2, 2, 64, 128),
        vmem(ROUNDS, 2, 2, 64, 128),
        vmem(ROUNDS, 2, 2, 8, 128),
        vmem(ROUNDS, 2, 2, 8, 128),
        vmem(ROUNDS, 2, 2, 2, 128),
        vmem(ROUNDS, 2, 2, 2, 128),
        vmem(1, 128),
        vmem(ny, 1, 128),
        vmem(1, 128),
        vmem(2 * nx, 1, 128),
        vmem(2, 8, 16),
        pltpu.SMEM((1,), F32),
        pltpu.SMEM((1,), F32),
        dma(6),
        dma(11),
        dma(11),
        dma(ROUNDS, 8),
        dma(ROUNDS, 8),
        dma(),
        dma(),
        dma(ny),
        dma(ny),
        dma(2 * nx),
        dma(2 * nx),
        pltpu.SemaphoreType.REGULAR((4,)),
        pltpu.SemaphoreType.REGULAR((4,)),
    ]
    anywhere = pl.BlockSpec(memory_space=pl.ANY)
    in_vmem = pl.BlockSpec(memory_space=pltpu.VMEM)
    in_smem = pl.BlockSpec(memory_space=pltpu.SMEM)
    result, line = pl.pallas_call(
        functools.partial(smoother, nx, ny),
        out_shape=(
            pltpu.VMEM(forcing.shape, F32),
            pltpu.SMEM((2,), F32),
        ),
        in_specs=[anywhere] * 6,
        out_specs=(in_vmem, in_smem),
        scratch_shapes=scratch,
        compiler_params=pltpu.CompilerParams(collective_id=0, has_side_effects=True),
    )(
        forcing,
        conductivity,
        lower_bound,
        upper_bound,
        jnp.asarray(bf16_tables(), BF16),
        jnp.asarray(f32_tables(), F32),
    )
    return result, line


def solution(mesh):
    spec = P("gx", "gy", "gz")
    return jax.shard_map(
        functools.partial(per_device, mesh.shape["gx"], mesh.shape["gy"]),
        mesh=mesh,
        in_specs=(spec, spec, P(), P()),
        out_specs=(spec, P()),
        check_vma=False,
    )
```
